32 devices in a mesh: tm: 4 (over y, core), lat: 8 (over z, x).
Axes of the slice: x: 2, y: 2, z: 4, core: 2. Of those that a mesh axis runs over, the one named last changes fastest.
Arguments:
- trajectory: float32 [4, 32, 64, 2048], P('tm', 'lat'), may hold values from -6 to 6
- diffusivity: float32 [4, 32, 64, 2048], P('tm', 'lat'), may hold values from 0.02 to 0.24
- adjoint_end: bfloat16 [32, 64, 2048], P('lat'), may hold values from -6 to 6
- obs_jac: bfloat16 [3072, 128, 128], P(('tm', 'lat')), may hold values from -0.5 to 0.5
- obs_value: float32 [3072, 128], P(('tm', 'lat')), may hold values from -6 to 6
- obs_weight: float32 [3072, 128], P(('tm', 'lat')), may hold values from 0.3 to 3
- obs_valid: int32 [3072, 128], P(('tm', 'lat')), may hold values 0 or 1
- obs_owner: int32 [3072, 1], P(('tm', 'lat')), may hold values from 0 to 31; in each aligned block of 96 rows (0 to 95, 96 to 191, ...) at most 6 rows name the same one
- obs_tile: int32 [3072], P(('tm', 'lat')), may hold values from 0 to 4095
Outputs:
- adjoint: float32 [4, 32, 64, 2048], P('tm', 'lat')
The draws below stay inside these ranges and needn't reach their ends.
Inputs may be any that keep to these rules, and one draw needn't show every extreme that they name: `obs_owner`: among the 96 blocks of one device, no owner is named more than 6 times, a bound that some block reaches.
All inputs are finite; a program needn't handle non-finite values. No bound on the sum of `obs_valid` on one device may be relied on, other than what follows from the above.
Results may differ from the reference program's by a relative error of at most 0.0024.
Values may be sent and summed in bfloat16 or wider, within the bound.
A program may use at most 128 MiB of HBM per device.

```python
import math
import jax
import jax.numpy as jnp
import numpy as np
from jax import lax

NLON = 2048
LEV = 64
TW = 2
CH = 128
SUB = 2
NB_DEV = 96
SECTIONS = 4
NLAT = 32
TILE = 128
TILES_DEV = 4096
CAP = 6
NOBS = 3072
N_LAT = 8
DEVICES = 32


def with_ends(entries, key, smallest, high):
    shape = entries.shape
    place = [jax.random.randint(jax.random.fold_in(key, axis), (), 0, shape[axis]) for axis in range(len(shape))]
    entries = entries.at[tuple(place)].set(smallest)
    longest = shape.index(max(shape))
    place[longest] = (place[longest] + 1) % shape[longest]
    return entries.at[tuple(place)].set(high)


def block_levels(rng, shape, cuts, least, largest):
    def one(dim, parts):
        draws = jax.random.uniform(jax.random.fold_in(jax.random.fold_in(rng, 6), dim), (parts,), jnp.float32, least / len(cuts), largest / len(cuts))
        return jnp.repeat(jnp.exp(draws), shape[dim] // parts).reshape((-1,) + (1,) * (len(shape) - dim - 1))

    loudness = one(*cuts[0])
    for cut in cuts[1:]:
        loudness = loudness * one(*cut)
    return loudness


def deal_out(key, own, number, rows, count, top, most, lean):
    sequence = jax.random.permutation(key, count)
    packed, ordinary = load_shares(count, rows * top, most, lean, True), load_shares(count, rows * top, most, lean, False)
    places = jnp.arange(count)

    def named(tallies, rotation):
        used = int((tallies > 0).sum())
        fixed = max(1, used // 4)
        shifted = fixed + (places - fixed + rotation * (used - fixed)) % max(1, count - fixed)
        return jnp.zeros((count,), jnp.int32).at[sequence[jnp.where(places < fixed, places, shifted)]].set(jnp.asarray(tallies, jnp.int32))

    tallies = jnp.where(number % 4 == 0, named(packed, number // 4), named(ordinary, number - number // 4 - 1))
    mixed = jax.random.permutation(jax.random.fold_in(own, 3), count)
    source_of, sink = mixed[0:count // 2 * 2:2], mixed[1:count // 2 * 2:2]
    slack = jnp.minimum(tallies[source_of] - 1, most - tallies[sink]) // 2
    slack = jnp.where((source_of == sequence[0]) | (sink == sequence[0]) | (tallies[sink] == 0), 0, jnp.maximum(slack, 0))
    shifted = jax.random.randint(jax.random.fold_in(own, 4), (count // 2,), 0, 1 << 20) % (slack + 1)
    tallies = tallies.at[source_of].add(-shifted).at[sink].add(shifted)
    labels = jnp.searchsorted(jnp.cumsum(tallies), jnp.arange(rows * top), side="right").astype(jnp.int32)
    grid = labels.reshape(top, rows).T
    grid = grid[jax.random.permutation(jax.random.fold_in(own, 1), rows)]
    rotation = jax.random.randint(jax.random.fold_in(own, 2), (rows, 1), 0, top)
    return jnp.take_along_axis(grid, (jnp.arange(top)[None, :] + rotation) % top, axis=1)


def load_shares(amount, total, most, slope, full):
    weights = [(1 << 20) // math.isqrt(standing ** slope) + 1 for standing in range(1, amount + 1)]
    largest = most if full else min(most, max(-(-total // amount), total * weights[0] // sum(weights)))
    least = 1 if total - largest >= amount - 1 else 0
    counts, surplus = [largest] + [least] * (amount - 1), total - largest - least * (amount - 1)
    while surplus > 0:
        movable = [i for i in range(1, amount) if counts[i] < largest] or [i for i in range(1, amount) if counts[i] < most]
        mass, remaining = sum([weights[i] for i in movable]), surplus
        for i in movable:
            more = min(most - counts[i], max(1, remaining * weights[i] // mass), surplus)
            counts[i] = counts[i] + more
            surplus = surplus - more
    return np.array(counts)


def gaussian(rng, shape, scale, most, shards=(), held_as=jnp.bfloat16):
    level = block_levels(rng, shape, shards, -0.22, 0.18) if shards else 1.0
    result = jax.random.normal(rng, shape, jnp.float32) * scale * level
    return jnp.minimum(jnp.maximum(result, -most), most).astype(held_as)


def setup_inputs(seed: int = 0) -> dict:
    streams_of = jax.random.split(jax.random.key(seed), 10)
    trajectory = gaussian(streams_of[0], (SECTIONS, NLAT, LEV, NLON), 1.0, 6.0, ((0, 4), (1, 8)), jnp.float32)
    diffusivity = jnp.clip(jnp.exp(math.log(0.24) - 2.4849066 * jax.random.uniform(streams_of[1], (SECTIONS, NLAT, LEV, NLON), jnp.float32) ** block_levels(streams_of[1], (SECTIONS, NLAT, LEV, NLON), ((0, 4), (1, 8)), -0.2, 0.2)), 0.02, 0.24)
    adjoint_end = gaussian(streams_of[2], (NLAT, LEV, NLON), 1.0, 6.0, ((0, 8),))
    obs_jac = gaussian(streams_of[3], (NOBS, CH, TILE), TILE ** -0.5, 0.5, ((0, 32),))
    obs_value = gaussian(streams_of[4], (NOBS, CH), 1.0, 6.0, ((0, 32),), jnp.float32)
    obs_weight = jnp.clip(jnp.exp(math.log(3.0) - 2.3025851 * jax.random.uniform(streams_of[5], (NOBS, CH), jnp.float32) ** block_levels(streams_of[5], (NOBS, CH), ((0, 32),), -0.2, 0.2)), 0.3, 3.0)
    obs_valid = with_ends((jax.random.randint(streams_of[6], (NOBS, CH), 0, 4) < 3).astype(jnp.int32), jax.random.fold_in(streams_of[6], 1), 0, 1)
    obs_owner_keys = jax.random.split(jax.random.fold_in(streams_of[7], 1), NOBS // NB_DEV)
    obs_owner_turns = jax.random.permutation(jax.random.fold_in(streams_of[7], 3), NOBS // NB_DEV)
    obs_owner = jax.vmap(lambda own, number: deal_out(jax.random.fold_in(streams_of[7], 2), own, number, NB_DEV, DEVICES, 1, CAP, 2))(obs_owner_keys, obs_owner_turns).reshape((NOBS, 1))
    obs_tile = with_ends(jax.random.randint(streams_of[8], (NOBS,), 0, TILES_DEV), jax.random.fold_in(streams_of[8], 1), 0, TILES_DEV - 1).astype(jnp.int32)
    return dict(trajectory=trajectory, diffusivity=diffusivity, adjoint_end=adjoint_end, obs_jac=obs_jac, obs_value=obs_value, obs_weight=obs_weight, obs_valid=obs_valid, obs_owner=obs_owner, obs_tile=obs_tile)


def spread(weighted):
    padded = jnp.pad(weighted, ((1, 1), (0, 0), (0, 0)))
    return padded[2:] + padded[:-2] + jnp.roll(weighted, 1, 2) + jnp.roll(weighted, -1, 2) - 4.0 * weighted


def propagate(field, kappa):
    for _ in range(SUB):
        field = field + spread(kappa * field)
    return field


def reference(trajectory, diffusivity, adjoint_end, obs_jac, obs_value, obs_weight, obs_valid, obs_owner, obs_tile):
    per_row = NLON // TW
    tiles = trajectory.reshape(SECTIONS, NLAT, LEV, per_row, TW).transpose(0, 1, 3, 2, 4).reshape(SECTIONS * NLAT * per_row, TILE)
    owner = obs_owner[:, 0]
    section = owner // N_LAT
    band = owner % N_LAT
    flat = (section * NLAT * per_row + band * TILES_DEV + obs_tile).astype(jnp.int32)
    states = tiles[flat]
    weights = obs_weight * obs_valid.astype(jnp.float32)

    def one(args):
        jac, state, value, weight = args
        jac_f = jac.astype(jnp.float32)
        pred = jnp.einsum("bct,bt->bc", jac_f, state, precision=lax.Precision.HIGHEST)
        resid = weight * (value - pred)
        return jnp.einsum("bct,bc->bt", jac_f, resid, precision=lax.Precision.HIGHEST)

    terms = lax.map(one, (obs_jac.reshape(DEVICES, NB_DEV, CH, TILE), states.reshape(DEVICES, NB_DEV, TILE),
                          obs_value.reshape(DEVICES, NB_DEV, CH), weights.reshape(DEVICES, NB_DEV, CH)))
    terms = terms.reshape(NOBS, TILE)
    forcing = jnp.zeros((SECTIONS * NLAT * per_row, TILE), jnp.float32).at[flat].add(terms)
    forcing = forcing.reshape(SECTIONS, NLAT, per_row, LEV, TW).transpose(0, 1, 3, 2, 4).reshape(SECTIONS, NLAT, LEV, NLON)
    results = [None] * SECTIONS
    current = adjoint_end.astype(jnp.float32)
    for section_id in range(SECTIONS - 1, -1, -1):
        if section_id == SECTIONS - 1:
            incoming = adjoint_end.astype(jnp.float32)
        else:
            incoming = lax.optimization_barrier(current.astype(jnp.bfloat16)).astype(jnp.float32)
        current = forcing[section_id] + propagate(incoming, diffusivity[section_id])
        results[section_id] = current
    return jnp.stack(results)
```

```python
import functools

import jax
import jax.numpy as jnp
from jax import lax
from jax.experimental import pallas as pl
from jax.experimental.pallas import tpu as pltpu
from jax.sharding import PartitionSpec as P

TW = 2
SUB = 2
LANES = 128
PAD = 8
CHUNK = 16
MESH = pl.DeviceIdType.MESH
VMEM = pl.BlockSpec(memory_space=pltpu.VMEM)
SMEM = pl.BlockSpec(memory_space=pltpu.SMEM)


def route_kernel(slots, owner_ref, tile_ref, ids_ref, slot_ref, count_ref):
    devices = ids_ref.shape[0]

    def clear(d, carry):
        count_ref[d] = 0
        for s in range(slots):
            ids_ref[d, s] = 0
        return carry

    lax.fori_loop(0, devices, clear, 0)

    def place(k, carry):
        target = owner_ref[k]
        rank = count_ref[target]
        count_ref[target] = rank + 1
        ids_ref[target, rank] = tile_ref[k]
        slot_ref[k] = target * PAD + rank
        return carry

    lax.fori_loop(0, owner_ref.shape[0], place, 0)


def route(owner, tile, devices, slots):
    return pl.pallas_call(
        functools.partial(route_kernel, slots),
        out_shape=(
            jax.ShapeDtypeStruct((devices, LANES), jnp.int32),
            jax.ShapeDtypeStruct(owner.shape, jnp.int32),
        ),
        in_specs=[SMEM, SMEM],
        out_specs=(SMEM, SMEM),
        scratch_shapes=[pltpu.SMEM((devices,), jnp.int32)],
        name="route",
    )(owner, tile)


def exchange_kernel(count, lat, x_ref, out_ref, send_sem, recv_sem, own_sem):
    me = lax.axis_index("tm") * lat + lax.axis_index("lat")
    barrier = pltpu.get_barrier_semaphore()

    def greet(j, carry):
        to = lax.rem(me + j, count)
        pl.semaphore_signal(barrier, inc=1, device_id=(to // lat, lax.rem(to, lat)), device_id_type=MESH)
        return carry

    lax.fori_loop(1, count, greet, 0)
    own = pltpu.make_async_copy(x_ref.at[me], out_ref.at[me], own_sem)
    own.start()
    pl.semaphore_wait(barrier, count - 1)

    def outgoing(j):
        to = lax.rem(me + j, count)
        return pltpu.make_async_remote_copy(
            src_ref=x_ref.at[to],
            dst_ref=out_ref.at[me],
            send_sem=send_sem.at[j],
            recv_sem=recv_sem.at[j],
            device_id=(to // lat, lax.rem(to, lat)),
            device_id_type=MESH,
        )

    def incoming(j):
        source = lax.rem(me + count - j, count)
        return pltpu.make_async_remote_copy(
            src_ref=x_ref.at[source],
            dst_ref=out_ref.at[source],
            send_sem=send_sem.at[j],
            recv_sem=recv_sem.at[j],
            device_id=(source // lat, lax.rem(source, lat)),
            device_id_type=MESH,
        )

    def launch(j, carry):
        outgoing(j).start()
        return carry

    def land(j, carry):
        incoming(j).wait_recv()
        outgoing(j).wait_send()
        return carry

    lax.fori_loop(1, count, launch, 0)
    own.wait()
    lax.fori_loop(1, count, land, 0)


def exchange(x, collective_id):
    lat = lax.axis_size("lat")
    count = lax.axis_size("tm") * lat
    return pl.pallas_call(
        functools.partial(exchange_kernel, count, lat),
        out_shape=jax.ShapeDtypeStruct(x.shape, x.dtype),
        in_specs=[VMEM],
        out_specs=VMEM,
        scratch_shapes=[
            pltpu.SemaphoreType.DMA((count,)),
            pltpu.SemaphoreType.DMA((count,)),
            pltpu.SemaphoreType.DMA,
        ],
        compiler_params=pltpu.CompilerParams(collective_id=collective_id, has_side_effects=True),
        name="exchange%d" % collective_id,
    )(x)


def tile_place(tile, per_row):
    row = tile // per_row
    lon = (tile - row * per_row) * TW
    column = lon // LANES
    return row, pl.multiple_of(column * LANES, LANES), lon - column * LANES


def gather_kernel(slots, ids_ref, traj_ref, out_ref):
    _, _, levels, nlon = traj_ref.shape
    per_row = nlon // TW
    tile_len = levels * TW
    entry = lax.broadcasted_iota(jnp.int32, (levels, tile_len), 1)
    level = lax.broadcasted_iota(jnp.int32, (levels, tile_len), 0)
    part = lax.rem(entry, TW)
    keep = entry // TW == level
    zeros = jnp.zeros((PAD - slots, tile_len), jnp.float32)

    def one(d, carry):
        rows = []
        for s in range(slots):
            row, start, offset = tile_place(ids_ref[d, s], per_row)
            field = traj_ref[0, row, :, pl.ds(start, LANES)]
            picked = jnp.take_along_axis(field, part + offset, axis=1)
            rows.append(jnp.sum(jnp.where(keep, picked, 0.0), axis=0, keepdims=True))
        out_ref[d] = jnp.concatenate(rows + [zeros], axis=0)
        return carry

    lax.fori_loop(0, out_ref.shape[0], one, 0)


def gather(ids, traj, slots):
    devices = ids.shape[0]
    tile_len = traj.shape[2] * TW
    return pl.pallas_call(
        functools.partial(gather_kernel, slots),
        out_shape=jax.ShapeDtypeStruct((devices, PAD, tile_len), jnp.float32),
        in_specs=[SMEM, VMEM],
        out_specs=VMEM,
        name="gather",
    )(ids, traj)


def split(x):
    top = x.astype(jnp.bfloat16)
    rest = (x - top.astype(jnp.float32)).astype(jnp.bfloat16)
    return jnp.concatenate([top, rest], axis=0)


def blocks_kernel(slot_ref, state_ref, jac_ref, value_ref, weight_ref, valid_ref, out_ref):
    group = PAD
    blocks, _, tile_len = jac_ref.shape
    out_ref[...] = jnp.zeros_like(out_ref)
    rank = lax.rem(lax.broadcasted_iota(jnp.int32, (2 * group, tile_len), 0), group)

    def product(vectors, first, dims):
        both = split(vectors)
        picked = jnp.zeros((2 * group, tile_len), jnp.float32)
        for i in range(group):
            full = lax.dot_general(both, jac_ref[first + i], dims, preferred_element_type=jnp.float32)
            picked = jnp.where(rank == i, full, picked)
        return picked[:group] + picked[group:]

    def one(g, carry):
        first = pl.multiple_of(g * group, group)
        places = [slot_ref[first + i] for i in range(group)]
        states = jnp.concatenate([state_ref[pl.ds(p, 1), :] for p in places], axis=0)
        here = pl.ds(first, group)
        pred = product(states, first, (((1,), (1,)), ((), ())))
        weight = weight_ref[here, :] * valid_ref[here, :].astype(jnp.float32)
        terms = product(weight * (value_ref[here, :] - pred), first, (((1,), (0,)), ((), ())))
        for i, p in enumerate(places):
            out_ref[pl.ds(p, 1), :] = terms[i : i + 1]
        return carry

    lax.fori_loop(0, blocks // group, one, 0)


def block_terms(slot, states, jac, value, weight, valid):
    return pl.pallas_call(
        blocks_kernel,
        out_shape=jax.ShapeDtypeStruct(states.shape, jnp.float32),
        in_specs=[SMEM] + [VMEM] * 5,
        out_specs=VMEM,
        name="blocks",
    )(slot, states, jac, value, weight, valid)


def scatter_kernel(slots, ids_ref, terms_ref, out_ref):
    _, levels, nlon = out_ref.shape
    per_row = nlon // TW
    out_ref[...] = jnp.zeros_like(out_ref)
    lane = lax.broadcasted_iota(jnp.int32, (levels, LANES), 1)
    level = lax.broadcasted_iota(jnp.int32, (levels, LANES), 0)
    source = level * TW + lax.rem(lane, TW)
    owner = lane // TW

    def one(d, carry):
        for s in range(slots):
            row, start, offset = tile_place(ids_ref[d, s], per_row)
            spread = jnp.broadcast_to(terms_ref[d, s : s + 1, :], (levels, levels * TW))
            moved = jnp.take_along_axis(spread, source, axis=1)
            here = (row, slice(None), pl.ds(start, LANES))
            out_ref[here] = out_ref[here] + jnp.where(owner == offset // TW, moved, 0.0)
        return carry

    lax.fori_loop(0, terms_ref.shape[0], one, 0)


def scatter(ids, terms, shape, slots):
    return pl.pallas_call(
        functools.partial(scatter_kernel, slots),
        out_shape=jax.ShapeDtypeStruct(shape, jnp.float32),
        in_specs=[SMEM, VMEM],
        out_specs=VMEM,
        name="scatter",
    )(ids, terms)


def chain_kernel(
    sections, lats, coeff_ref, low_ref, high_ref, end_ref, forcing_ref, out_ref,
    main, low, high, ahead, first_buf, second_buf,
    main_send, main_recv, down_send, up_send, low_recv, high_recv,
):
    section, band = lax.axis_index("tm"), lax.axis_index("lat")
    rows, levels, nlon = end_ref.shape
    chunks = levels // CHUNK
    is_last = section == sections - 1
    has_before, has_low, has_high = section > 0, band > 0, band < lats - 1

    barrier = pltpu.get_barrier_semaphore()
    sides = (
        (jnp.logical_not(is_last), section + 1, band),
        (has_before, section - 1, band),
        (has_low, section, band - 1),
        (has_high, section, band + 1),
    )
    for there, tm, lat in sides:
        @pl.when(there)
        def _(tm=tm, lat=lat):
            pl.semaphore_signal(barrier, inc=1, device_id=(tm, lat), device_id_type=MESH)
    pl.semaphore_wait(barrier, sum(there.astype(jnp.int32) for there, _, _ in sides))

    def remote(src, dst, send, recv, tm, lat):
        return pltpu.make_async_remote_copy(
            src_ref=src, dst_ref=dst, send_sem=send, recv_sem=recv, device_id=(tm, lat), device_id_type=MESH
        )

    def local_main(c):
        return pltpu.make_async_copy(
            end_ref.at[:, pl.ds(pl.multiple_of(c * CHUNK, CHUNK), CHUNK), :], main.at[c], main_recv.at[c]
        )

    def handed(c):
        return remote(ahead.at[c], main.at[c], main_send.at[c], main_recv.at[c], section - 1, band)

    def downward(c):
        return remote(main.at[c, pl.ds(0, SUB)], high.at[c], down_send.at[c], high_recv.at[c], section, band - 1)

    def upward(c):
        return remote(main.at[c, pl.ds(rows - SUB, SUB)], low.at[c], up_send.at[c], low_recv.at[c], section, band + 1)

    @pl.when(jnp.logical_not(has_low))
    def _():
        low[...] = jnp.zeros_like(low)

    @pl.when(jnp.logical_not(has_high))
    def _():
        high[...] = jnp.zeros_like(high)

    @pl.when(is_last)
    def _():
        for c in range(chunks):
            local_main(c).start()

    def pass_edges(c):
        @pl.when(is_last)
        def _():
            local_main(c).wait()

        @pl.when(jnp.logical_not(is_last))
        def _():
            handed(c).wait_recv()

        @pl.when(has_low)
        def _():
            downward(c).start()

        @pl.when(has_high)
        def _():
            upward(c).start()

    def compute(c):
        span = pl.ds(pl.multiple_of(c * CHUNK, CHUNK), CHUNK)
        total = rows + 2 * SUB

        def field(i):
            if i < SUB:
                return low[c, i].astype(jnp.float32)
            if i < SUB + rows:
                return main[c, i - SUB].astype(jnp.float32)
            return high[c, i - SUB - rows].astype(jnp.float32)

        def coeff(i):
            if i < SUB:
                return low_ref[i, span, :].astype(jnp.float32)
            if i < SUB + rows:
                return coeff_ref[0, i - SUB, span, :]
            return high_ref[i - SUB - rows, span, :].astype(jnp.float32)

        def spread(buf, i):
            mid = buf[i]
            return buf[i + 1] + buf[i - 1] + pltpu.roll(mid, 1, 1) + pltpu.roll(mid, nlon - 1, 1) - 4.0 * mid

        for i in range(total):
            first_buf[i] = coeff(i) * field(i)
        for i in range(1, total - 1):
            value = field(i) + spread(first_buf, i)
            second_buf[i] = coeff(i) * value
            if SUB <= i < SUB + rows:
                out_ref[0, i - SUB, span, :] = forcing_ref[i - SUB, span, :] + value
        for r in range(rows):
            value = out_ref[0, r, span, :] + spread(second_buf, r + SUB)
            out_ref[0, r, span, :] = value
            ahead[c, r] = value.astype(jnp.bfloat16)

    pass_edges(0)

    def step(c, carry):
        @pl.when(c + 1 < chunks)
        def _():
            pass_edges(c + 1)

        @pl.when(has_low)
        def _():
            upward(c).wait_recv()

        @pl.when(has_high)
        def _():
            downward(c).wait_recv()

        compute(c)

        @pl.when(has_before)
        def _():
            handed(c).start()

        return carry

    lax.fori_loop(0, chunks, step, 0)

    def finish(c, carry):
        @pl.when(has_low)
        def _():
            downward(c).wait_send()

        @pl.when(has_high)
        def _():
            upward(c).wait_send()

        @pl.when(has_before)
        def _():
            handed(c).wait_send()

        return carry

    lax.fori_loop(0, chunks, finish, 0)


def chain(coeff, low, high, end, forcing):
    rows, levels, nlon = end.shape
    chunks = levels // CHUNK
    part = lambda n, kind: pltpu.VMEM((chunks, n, CHUNK, nlon), kind)
    whole = pltpu.VMEM((rows + 2 * SUB, CHUNK, nlon), jnp.float32)
    return pl.pallas_call(
        functools.partial(chain_kernel, lax.axis_size("tm"), lax.axis_size("lat")),
        out_shape=jax.ShapeDtypeStruct(coeff.shape, jnp.float32),
        in_specs=[VMEM] * 5,
        out_specs=VMEM,
        scratch_shapes=[
            part(rows, jnp.bfloat16),
            part(SUB, jnp.bfloat16),
            part(SUB, jnp.bfloat16),
            part(rows, jnp.bfloat16),
            whole,
            whole,
        ]
        + [pltpu.SemaphoreType.DMA((chunks,))] * 6,
        compiler_params=pltpu.CompilerParams(
            collective_id=9, has_side_effects=True, vmem_limit_bytes=48 * 1024 * 1024
        ),
        name="chain",
    )(coeff, low, high, end, forcing)


def per_device(
    trajectory,
    diffusivity,
    adjoint_end,
    obs_jac,
    obs_value,
    obs_weight,
    obs_valid,
    obs_owner,
    obs_tile,
):
    _, lat_dev, levels, nlon = trajectory.shape
    lats = lax.axis_size("lat")
    devices = lax.axis_size("tm") * lats
    blocks = obs_owner.shape[0]
    slots = max(2, 2 * blocks // devices)
    upward = [(i, i + 1) for i in range(lats - 1)]
    downward = [(i + 1, i) for i in range(lats - 1)]
    low = lax.ppermute(diffusivity[0, lat_dev - SUB :].astype(jnp.bfloat16), "lat", upward)
    high = lax.ppermute(diffusivity[0, :SUB].astype(jnp.bfloat16), "lat", downward)

    ids, slot = route(obs_owner[:, 0], obs_tile, devices, slots)
    wanted = exchange(ids[:, None, :], 1)[:, 0]
    found = gather(wanted, trajectory, slots)
    returned = exchange(found, 2)
    terms = block_terms(
        slot, returned.reshape(devices * PAD, -1), obs_jac, obs_value, obs_weight, obs_valid
    )
    received = exchange(terms.reshape(found.shape), 3)
    forcing = scatter(wanted, received, (lat_dev, levels, nlon), slots)
    return chain(diffusivity, low, high, adjoint_end, forcing)


def solution(mesh):
    in_specs = (
        P("tm", "lat", None, None),
        P("tm", "lat", None, None),
        P("lat", None, None),
        P(("tm", "lat"), None, None),
        P(("tm", "lat"), None),
        P(("tm", "lat"), None),
        P(("tm", "lat"), None),
        P(("tm", "lat"), None),
        P(("tm", "lat")),
    )
    out_specs = P("tm", "lat", None, None)
    return jax.shard_map(
        per_device, mesh=mesh, in_specs=in_specs, out_specs=out_specs, check_vma=False
    )
```

```python
import functools

import jax
import jax.numpy as jnp
from jax import lax
from jax.experimental import pallas as pl
from jax.experimental.pallas import tpu as pltpu
from jax.sharding import PartitionSpec as P

TW = 2
SUB = 2
LANES = 128
PAD = 8
CHUNK = 16
MESH = pl.DeviceIdType.MESH
VMEM = pl.BlockSpec(memory_space=pltpu.VMEM)
SMEM = pl.BlockSpec(memory_space=pltpu.SMEM)


def route_kernel(slots, owner_ref, tile_ref, ids_ref, slot_ref, count_ref):
    devices = ids_ref.shape[0]

    def clear(d, carry):
        count_ref[d] = 0
        for s in range(slots):
            ids_ref[d, s] = 0
        return carry

    lax.fori_loop(0, devices, clear, 0)

    def place(k, carry):
        target = owner_ref[k]
        rank = count_ref[target]
        count_ref[target] = rank + 1
        ids_ref[target, rank] = tile_ref[k]
        slot_ref[k] = target * PAD + rank
        return carry

    lax.fori_loop(0, owner_ref.shape[0], place, 0)


def route(owner, tile, devices, slots):
    return pl.pallas_call(
        functools.partial(route_kernel, slots),
        out_shape=(
            jax.ShapeDtypeStruct((devices, LANES), jnp.int32),
            jax.ShapeDtypeStruct(owner.shape, jnp.int32),
        ),
        in_specs=[SMEM, SMEM],
        out_specs=(SMEM, SMEM),
        scratch_shapes=[pltpu.SMEM((devices,), jnp.int32)],
        name="route",
    )(owner, tile)


def exchange_kernel(count, lat, x_ref, out_ref, send_sem, recv_sem, own_sem):
    me = lax.axis_index("tm") * lat + lax.axis_index("lat")
    barrier = pltpu.get_barrier_semaphore()

    def greet(j, carry):
        to = lax.rem(me + j, count)
        pl.semaphore_signal(barrier, inc=1, device_id=(to // lat, lax.rem(to, lat)), device_id_type=MESH)
        return carry

    lax.fori_loop(1, count, greet, 0)
    own = pltpu.make_async_copy(x_ref.at[me], out_ref.at[me], own_sem)
    own.start()
    pl.semaphore_wait(barrier, count - 1)

    def outgoing(j):
        to = lax.rem(me + j, count)
        return pltpu.make_async_remote_copy(
            src_ref=x_ref.at[to],
            dst_ref=out_ref.at[me],
            send_sem=send_sem.at[j],
            recv_sem=recv_sem.at[j],
            device_id=(to // lat, lax.rem(to, lat)),
            device_id_type=MESH,
        )

    def incoming(j):
        source = lax.rem(me + count - j, count)
        return pltpu.make_async_remote_copy(
            src_ref=x_ref.at[source],
            dst_ref=out_ref.at[source],
            send_sem=send_sem.at[j],
            recv_sem=recv_sem.at[j],
            device_id=(source // lat, lax.rem(source, lat)),
            device_id_type=MESH,
        )

    def launch(j, carry):
        outgoing(j).start()
        return carry

    def land(j, carry):
        incoming(j).wait_recv()
        outgoing(j).wait_send()
        return carry

    lax.fori_loop(1, count, launch, 0)
    own.wait()
    lax.fori_loop(1, count, land, 0)


def exchange(x, collective_id):
    lat = lax.axis_size("lat")
    count = lax.axis_size("tm") * lat
    return pl.pallas_call(
        functools.partial(exchange_kernel, count, lat),
        out_shape=jax.ShapeDtypeStruct(x.shape, x.dtype),
        in_specs=[VMEM],
        out_specs=VMEM,
        scratch_shapes=[
            pltpu.SemaphoreType.DMA((count,)),
            pltpu.SemaphoreType.DMA((count,)),
            pltpu.SemaphoreType.DMA,
        ],
        compiler_params=pltpu.CompilerParams(collective_id=collective_id, has_side_effects=True),
        name="exchange%d" % collective_id,
    )(x)


def tile_place(tile, per_row):
    row = tile // per_row
    lon = (tile - row * per_row) * TW
    column = lon // LANES
    return row, pl.multiple_of(column * LANES, LANES), lon - column * LANES


def gather_kernel(slots, ids_ref, traj_ref, out_ref):
    _, _, levels, nlon = traj_ref.shape
    per_row = nlon // TW
    tile_len = levels * TW
    entry = lax.broadcasted_iota(jnp.int32, (levels, tile_len), 1)
    level = lax.broadcasted_iota(jnp.int32, (levels, tile_len), 0)
    part = lax.rem(entry, TW)
    keep = entry // TW == level
    zeros = jnp.zeros((PAD - slots, tile_len), jnp.float32)

    def one(d, carry):
        rows = []
        for s in range(slots):
            row, start, offset = tile_place(ids_ref[d, s], per_row)
            field = traj_ref[0, row, :, pl.ds(start, LANES)]
            picked = jnp.take_along_axis(field, part + offset, axis=1)
            rows.append(jnp.sum(jnp.where(keep, picked, 0.0), axis=0, keepdims=True))
        out_ref[d] = jnp.concatenate(rows + [zeros], axis=0)
        return carry

    lax.fori_loop(0, out_ref.shape[0], one, 0)


def gather(ids, traj, slots):
    devices = ids.shape[0]
    tile_len = traj.shape[2] * TW
    return pl.pallas_call(
        functools.partial(gather_kernel, slots),
        out_shape=jax.ShapeDtypeStruct((devices, PAD, tile_len), jnp.float32),
        in_specs=[SMEM, VMEM],
        out_specs=VMEM,
        name="gather",
    )(ids, traj)


def split(x):
    top = x.astype(jnp.bfloat16)
    rest = (x - top.astype(jnp.float32)).astype(jnp.bfloat16)
    return jnp.concatenate([top, rest], axis=0)


def blocks_kernel(slot_ref, state_ref, jac_ref, value_ref, weight_ref, valid_ref, out_ref):
    group = PAD
    blocks, _, tile_len = jac_ref.shape
    out_ref[...] = jnp.zeros_like(out_ref)
    rank = lax.rem(lax.broadcasted_iota(jnp.int32, (2 * group, tile_len), 0), group)

    def product(vectors, first, dims):
        both = split(vectors)
        picked = jnp.zeros((2 * group, tile_len), jnp.float32)
        for i in range(group):
            full = lax.dot_general(both, jac_ref[first + i], dims, preferred_element_type=jnp.float32)
            picked = jnp.where(rank == i, full, picked)
        return picked[:group] + picked[group:]

    def one(g, carry):
        first = pl.multiple_of(g * group, group)
        places = [slot_ref[first + i] for i in range(group)]
        states = jnp.concatenate([state_ref[pl.ds(p, 1), :] for p in places], axis=0)
        here = pl.ds(first, group)
        pred = product(states, first, (((1,), (1,)), ((), ())))
        weight = weight_ref[here, :] * valid_ref[here, :].astype(jnp.float32)
        terms = product(weight * (value_ref[here, :] - pred), first, (((1,), (0,)), ((), ())))
        for i, p in enumerate(places):
            out_ref[pl.ds(p, 1), :] = terms[i : i + 1]
        return carry

    lax.fori_loop(0, blocks // group, one, 0)


def block_terms(slot, states, jac, value, weight, valid):
    return pl.pallas_call(
        blocks_kernel,
        out_shape=jax.ShapeDtypeStruct(states.shape, jnp.float32),
        in_specs=[SMEM] + [VMEM] * 5,
        out_specs=VMEM,
        name="blocks",
    )(slot, states, jac, value, weight, valid)


def scatter_kernel(slots, ids_ref, terms_ref, out_ref):
    _, levels, nlon = out_ref.shape
    per_row = nlon // TW
    out_ref[...] = jnp.zeros_like(out_ref)
    lane = lax.broadcasted_iota(jnp.int32, (levels, LANES), 1)
    level = lax.broadcasted_iota(jnp.int32, (levels, LANES), 0)
    source = level * TW + lax.rem(lane, TW)
    owner = lane // TW

    def one(d, carry):
        for s in range(slots):
            row, start, offset = tile_place(ids_ref[d, s], per_row)
            spread = jnp.broadcast_to(terms_ref[d, s : s + 1, :], (levels, levels * TW))
            moved = jnp.take_along_axis(spread, source, axis=1)
            here = (row, slice(None), pl.ds(start, LANES))
            out_ref[here] = out_ref[here] + jnp.where(owner == offset // TW, moved, 0.0)
        return carry

    lax.fori_loop(0, terms_ref.shape[0], one, 0)


def scatter(ids, terms, shape, slots):
    return pl.pallas_call(
        functools.partial(scatter_kernel, slots),
        out_shape=jax.ShapeDtypeStruct(shape, jnp.float32),
        in_specs=[SMEM, VMEM],
        out_specs=VMEM,
        name="scatter",
    )(ids, terms)


def chain_kernel(
    sections, lats, coeff_ref, low_ref, high_ref, end_ref, forcing_ref, out_ref,
    main, low, high, edge_low, edge_high, ahead, weighted, partial, second,
    main_send, main_recv, down_send, up_send, low_recv, high_recv,
):
    section, band = lax.axis_index("tm"), lax.axis_index("lat")
    rows, levels, nlon = end_ref.shape
    chunks = levels // CHUNK
    is_last = section == sections - 1
    has_before, has_low, has_high = section > 0, band > 0, band < lats - 1

    barrier = pltpu.get_barrier_semaphore()
    sides = (
        (jnp.logical_not(is_last), section + 1, band),
        (has_before, section - 1, band),
        (has_low, section, band - 1),
        (has_high, section, band + 1),
    )
    for there, tm, lat in sides:
        @pl.when(there)
        def _(tm=tm, lat=lat):
            pl.semaphore_signal(barrier, inc=1, device_id=(tm, lat), device_id_type=MESH)
    pl.semaphore_wait(barrier, sum(there.astype(jnp.int32) for there, _, _ in sides))

    def remote(src, dst, send, recv, tm, lat):
        return pltpu.make_async_remote_copy(
            src_ref=src, dst_ref=dst, send_sem=send, recv_sem=recv, device_id=(tm, lat), device_id_type=MESH
        )

    def local_main(c):
        return pltpu.make_async_copy(
            end_ref.at[:, pl.ds(pl.multiple_of(c * CHUNK, CHUNK), CHUNK), :], main.at[c], main_recv.at[c]
        )

    def handed(c):
        return remote(ahead.at[c], main.at[c], main_send.at[c], main_recv.at[c], section - 1, band)

    def downward(c):
        return remote(edge_low.at[c], high.at[c], down_send.at[c], high_recv.at[c], section, band - 1)

    def upward(c):
        return remote(edge_high.at[c], low.at[c], up_send.at[c], low_recv.at[c], section, band + 1)

    @pl.when(jnp.logical_not(has_low))
    def _():
        low[...] = jnp.zeros_like(low)

    @pl.when(jnp.logical_not(has_high))
    def _():
        high[...] = jnp.zeros_like(high)

    @pl.when(is_last)
    def _():
        for c in range(chunks):
            local_main(c).start()

    def levels_of(c):
        return pl.ds(pl.multiple_of(c * CHUNK, CHUNK), CHUNK)

    def along(mid):
        return pltpu.roll(mid, 1, 1) + pltpu.roll(mid, nlon - 1, 1) - 4.0 * mid

    def begin(c):
        @pl.when(is_last)
        def _():
            local_main(c).wait()

        @pl.when(jnp.logical_not(is_last))
        def _():
            handed(c).wait_recv()

        span = levels_of(c)
        for r in range(rows):
            weighted[c, r] = coeff_ref[0, r, span, :] * main[c, r].astype(jnp.float32)
        for r in range(rows):
            mid = weighted[c, r]
            value = main[c, r].astype(jnp.float32) + along(mid)
            if r > 0:
                value = value + weighted[c, r - 1]
            if r < rows - 1:
                value = value + weighted[c, r + 1]
            partial[c, r] = value
            if r == 0:
                edge_low[c, 0] = mid.astype(jnp.bfloat16)
                edge_low[c, 1] = (coeff_ref[0, r, span, :] * value).astype(jnp.bfloat16)
            if r == rows - 1:
                edge_high[c, 0] = mid.astype(jnp.bfloat16)
                edge_high[c, 1] = (coeff_ref[0, r, span, :] * value).astype(jnp.bfloat16)

        @pl.when(has_low)
        def _():
            downward(c).start()

        @pl.when(has_high)
        def _():
            upward(c).start()

    def complete(c):
        span = levels_of(c)
        end = rows - 1
        partial[c, 0] = partial[c, 0] + low[c, 0].astype(jnp.float32)
        partial[c, end] = partial[c, end] + high[c, 0].astype(jnp.float32)
        second[0] = low[c, 1].astype(jnp.float32) + low_ref[0, span, :].astype(jnp.float32) * weighted[c, 0]
        second[rows + 1] = high[c, 1].astype(jnp.float32) + high_ref[0, span, :].astype(jnp.float32) * weighted[c, end]
        for r in range(rows):
            second[r + 1] = coeff_ref[0, r, span, :] * partial[c, r]
        for r in range(rows):
            value = partial[c, r] + second[r] + second[r + 2] + along(second[r + 1]) + forcing_ref[r, span, :]
            out_ref[0, r, span, :] = value
            ahead[c, r] = value.astype(jnp.bfloat16)

    begin(0)

    def step(c, carry):
        @pl.when(c + 1 < chunks)
        def _():
            begin(c + 1)

        @pl.when(has_low)
        def _():
            upward(c).wait_recv()

        @pl.when(has_high)
        def _():
            downward(c).wait_recv()

        complete(c)

        @pl.when(has_before)
        def _():
            handed(c).start()

        return carry

    lax.fori_loop(0, chunks, step, 0)

    def finish(c, carry):
        @pl.when(has_low)
        def _():
            downward(c).wait_send()

        @pl.when(has_high)
        def _():
            upward(c).wait_send()

        @pl.when(has_before)
        def _():
            handed(c).wait_send()

        return carry

    lax.fori_loop(0, chunks, finish, 0)


def chain(coeff, low, high, end, forcing):
    rows, levels, nlon = end.shape
    chunks = levels // CHUNK
    part = lambda n, kind: pltpu.VMEM((chunks, n, CHUNK, nlon), kind)
    return pl.pallas_call(
        functools.partial(chain_kernel, lax.axis_size("tm"), lax.axis_size("lat")),
        out_shape=jax.ShapeDtypeStruct(coeff.shape, jnp.float32),
        in_specs=[VMEM] * 5,
        out_specs=VMEM,
        scratch_shapes=[
            part(rows, jnp.bfloat16),
            part(SUB, jnp.bfloat16),
            part(SUB, jnp.bfloat16),
            part(SUB, jnp.bfloat16),
            part(SUB, jnp.bfloat16),
            part(rows, jnp.bfloat16),
            part(rows, jnp.float32),
            part(rows, jnp.float32),
            pltpu.VMEM((rows + 2, CHUNK, nlon), jnp.float32),
        ]
        + [pltpu.SemaphoreType.DMA((chunks,))] * 6,
        compiler_params=pltpu.CompilerParams(
            collective_id=9, has_side_effects=True, vmem_limit_bytes=48 * 1024 * 1024
        ),
        name="chain",
    )(coeff, low, high, end, forcing)


def per_device(
    trajectory,
    diffusivity,
    adjoint_end,
    obs_jac,
    obs_value,
    obs_weight,
    obs_valid,
    obs_owner,
    obs_tile,
):
    _, lat_dev, levels, nlon = trajectory.shape
    lats = lax.axis_size("lat")
    devices = lax.axis_size("tm") * lats
    blocks = obs_owner.shape[0]
    slots = max(2, 2 * blocks // devices)
    upward = [(i, i + 1) for i in range(lats - 1)]
    downward = [(i + 1, i) for i in range(lats - 1)]
    ids, slot = route(obs_owner[:, 0], obs_tile, devices, slots)
    wanted = exchange(ids[:, None, :], 1)[:, 0]
    edges = lax.optimization_barrier((diffusivity[0, :1], diffusivity[0, lat_dev - 1 :], wanted))
    wanted = edges[2]
    low = lax.ppermute(edges[1].astype(jnp.bfloat16), "lat", upward)
    high = lax.ppermute(edges[0].astype(jnp.bfloat16), "lat", downward)
    found = gather(wanted, trajectory, slots)
    returned = exchange(found, 2)
    terms = block_terms(
        slot, returned.reshape(devices * PAD, -1), obs_jac, obs_value, obs_weight, obs_valid
    )
    received = exchange(terms.reshape(found.shape), 3)
    forcing = scatter(wanted, received, (lat_dev, levels, nlon), slots)
    return chain(diffusivity, low, high, adjoint_end, forcing)


def solution(mesh):
    in_specs = (
        P("tm", "lat", None, None),
        P("tm", "lat", None, None),
        P("lat", None, None),
        P(("tm", "lat"), None, None),
        P(("tm", "lat"), None),
        P(("tm", "lat"), None),
        P(("tm", "lat"), None),
        P(("tm", "lat"), None),
        P(("tm", "lat")),
    )
    out_specs = P("tm", "lat", None, None)
    return jax.shard_map(
        per_device, mesh=mesh, in_specs=in_specs, out_specs=out_specs, check_vma=False
    )
```

```python
import functools

import jax
import jax.numpy as jnp
from jax import lax
from jax.experimental import pallas as pl
from jax.experimental.pallas import tpu as pltpu
from jax.sharding import PartitionSpec as P

TW = 2
SUB = 2
LANES = 128
PAD = 8
CHUNK = 8
MESH = pl.DeviceIdType.MESH
VMEM = pl.BlockSpec(memory_space=pltpu.VMEM)
SMEM = pl.BlockSpec(memory_space=pltpu.SMEM)


def route_kernel(slots, owner_ref, tile_ref, ids_ref, slot_ref, count_ref):
    devices = ids_ref.shape[0]

    def clear(d, carry):
        count_ref[d] = 0
        for s in range(slots):
            ids_ref[d, s] = 0
        return carry

    lax.fori_loop(0, devices, clear, 0)

    def place(k, carry):
        target = owner_ref[k]
        rank = count_ref[target]
        count_ref[target] = rank + 1
        ids_ref[target, rank] = tile_ref[k]
        slot_ref[k] = target * PAD + rank
        return carry

    lax.fori_loop(0, owner_ref.shape[0], place, 0)


def route(owner, tile, devices, slots):
    return pl.pallas_call(
        functools.partial(route_kernel, slots),
        out_shape=(
            jax.ShapeDtypeStruct((devices, LANES), jnp.int32),
            jax.ShapeDtypeStruct(owner.shape, jnp.int32),
        ),
        in_specs=[SMEM, SMEM],
        out_specs=(SMEM, SMEM),
        scratch_shapes=[pltpu.SMEM((devices,), jnp.int32)],
        name="route",
    )(owner, tile)


def exchange_kernel(count, lat, shift, *refs):
    if shift:
        x_ref, edge_ref, out_ref, beside_ref, send_sem, recv_sem, own_sem, edge_send, edge_recv = refs
    else:
        x_ref, out_ref, send_sem, recv_sem, own_sem = refs
    me = lax.axis_index("tm") * lat + lax.axis_index("lat")
    barrier = pltpu.get_barrier_semaphore()

    def greet(j, carry):
        to = lax.rem(me + j, count)
        pl.semaphore_signal(barrier, inc=1, device_id=(to // lat, lax.rem(to, lat)), device_id_type=MESH)
        return carry

    lax.fori_loop(1, count, greet, 0)
    own = pltpu.make_async_copy(x_ref.at[me], out_ref.at[me], own_sem)
    own.start()
    pl.semaphore_wait(barrier, count - 1)

    def outgoing(j):
        to = lax.rem(me + j, count)
        return pltpu.make_async_remote_copy(
            src_ref=x_ref.at[to],
            dst_ref=out_ref.at[me],
            send_sem=send_sem.at[j],
            recv_sem=recv_sem.at[j],
            device_id=(to // lat, lax.rem(to, lat)),
            device_id_type=MESH,
        )

    def incoming(j):
        source = lax.rem(me + count - j, count)
        return pltpu.make_async_remote_copy(
            src_ref=x_ref.at[source],
            dst_ref=out_ref.at[source],
            send_sem=send_sem.at[j],
            recv_sem=recv_sem.at[j],
            device_id=(source // lat, lax.rem(source, lat)),
            device_id_type=MESH,
        )

    def launch(j, carry):
        outgoing(j).start()
        return carry

    def land(j, carry):
        incoming(j).wait_recv()
        outgoing(j).wait_send()
        return carry

    lax.fori_loop(1, count, launch, 0)
    if shift:
        band, section = lax.axis_index("lat"), lax.axis_index("tm")
        is_last = section == count // lat - 1
        gives = is_last & (band < lat - 1 if shift > 0 else band > 0)
        takes = is_last & (band > 0 if shift > 0 else band < lat - 1)

        def edge():
            return pltpu.make_async_remote_copy(
                src_ref=edge_ref,
                dst_ref=beside_ref,
                send_sem=edge_send,
                recv_sem=edge_recv,
                device_id=(section, band + shift),
                device_id_type=MESH,
            )

        @pl.when(gives)
        def _():
            edge().start()

        @pl.when(jnp.logical_not(takes))
        def _():
            beside_ref[...] = jnp.zeros_like(beside_ref)

    own.wait()
    lax.fori_loop(1, count, land, 0)
    if shift:
        @pl.when(takes)
        def _():
            edge().wait_recv()

        @pl.when(gives)
        def _():
            edge().wait_send()


def last_edges_kernel(coeff_ref, end_ref, low_ref, high_ref):
    rows, levels, nlon = end_ref.shape

    def one(c, carry):
        span = pl.ds(pl.multiple_of(c * 16, 16), 16)

        def weigh(r):
            return coeff_ref[0, r, span, :] * end_ref[r, span, :].astype(jnp.float32)

        for r, inner, ref in ((0, 1, low_ref), (rows - 1, rows - 2, high_ref)):
            mid = weigh(r)
            value = end_ref[r, span, :].astype(jnp.float32) + weigh(inner)
            value = value + pltpu.roll(mid, 1, 1) + pltpu.roll(mid, nlon - 1, 1) - 4.0 * mid
            ref[0, span, :] = mid.astype(jnp.bfloat16)
            ref[1, span, :] = (coeff_ref[0, r, span, :] * value).astype(jnp.bfloat16)
        return carry

    lax.fori_loop(0, levels // 16, one, 0)


def last_edges(coeff, end):
    edge = jax.ShapeDtypeStruct((2,) + end.shape[1:], jnp.bfloat16)
    return pl.pallas_call(
        last_edges_kernel,
        out_shape=(edge, edge),
        in_specs=[VMEM, VMEM],
        out_specs=(VMEM, VMEM),
        name="last_edges",
    )(coeff, end)


def exchange(x, collective_id, edge=None, shift=0):
    lat = lax.axis_size("lat")
    count = lax.axis_size("tm") * lat
    if shift:
        return pl.pallas_call(
            functools.partial(exchange_kernel, count, lat, shift),
            out_shape=(jax.ShapeDtypeStruct(x.shape, x.dtype), jax.ShapeDtypeStruct(edge.shape, edge.dtype)),
            in_specs=[VMEM, VMEM],
            out_specs=(VMEM, VMEM),
            scratch_shapes=[pltpu.SemaphoreType.DMA((count,))] * 2 + [pltpu.SemaphoreType.DMA] * 3,
            compiler_params=pltpu.CompilerParams(collective_id=collective_id, has_side_effects=True),
            name="exchange%d" % collective_id,
        )(x, edge)
    return pl.pallas_call(
        functools.partial(exchange_kernel, count, lat, 0),
        out_shape=jax.ShapeDtypeStruct(x.shape, x.dtype),
        in_specs=[VMEM],
        out_specs=VMEM,
        scratch_shapes=[
            pltpu.SemaphoreType.DMA((count,)),
            pltpu.SemaphoreType.DMA((count,)),
            pltpu.SemaphoreType.DMA,
        ],
        compiler_params=pltpu.CompilerParams(collective_id=collective_id, has_side_effects=True),
        name="exchange%d" % collective_id,
    )(x)


def tile_place(tile, per_row):
    row = tile // per_row
    lon = (tile - row * per_row) * TW
    column = lon // LANES
    return row, pl.multiple_of(column * LANES, LANES), lon - column * LANES


def gather_kernel(slots, ids_ref, traj_ref, out_ref):
    _, _, levels, nlon = traj_ref.shape
    per_row = nlon // TW
    tile_len = levels * TW
    entry = lax.broadcasted_iota(jnp.int32, (levels, tile_len), 1)
    level = lax.broadcasted_iota(jnp.int32, (levels, tile_len), 0)
    part = lax.rem(entry, TW)
    keep = entry // TW == level
    zeros = jnp.zeros((PAD - slots, tile_len), jnp.float32)

    def one(d, carry):
        rows = []
        for s in range(slots):
            row, start, offset = tile_place(ids_ref[d, s], per_row)
            field = traj_ref[0, row, :, pl.ds(start, LANES)]
            picked = jnp.take_along_axis(field, part + offset, axis=1)
            rows.append(jnp.sum(jnp.where(keep, picked, 0.0), axis=0, keepdims=True))
        out_ref[d] = jnp.concatenate(rows + [zeros], axis=0)
        return carry

    lax.fori_loop(0, out_ref.shape[0], one, 0)


def gather(ids, traj, slots):
    devices = ids.shape[0]
    tile_len = traj.shape[2] * TW
    return pl.pallas_call(
        functools.partial(gather_kernel, slots),
        out_shape=jax.ShapeDtypeStruct((devices, PAD, tile_len), jnp.float32),
        in_specs=[SMEM, VMEM],
        out_specs=VMEM,
        name="gather",
    )(ids, traj)


def split(x):
    top = x.astype(jnp.bfloat16)
    rest = (x - top.astype(jnp.float32)).astype(jnp.bfloat16)
    return jnp.concatenate([top, rest], axis=0)


def blocks_kernel(slot_ref, state_ref, jac_ref, value_ref, weight_ref, valid_ref, out_ref):
    group = PAD
    blocks, _, tile_len = jac_ref.shape
    out_ref[...] = jnp.zeros_like(out_ref)
    rank = lax.rem(lax.broadcasted_iota(jnp.int32, (2 * group, tile_len), 0), group)

    def product(vectors, first, dims):
        both = split(vectors)
        picked = jnp.zeros((2 * group, tile_len), jnp.float32)
        for i in range(group):
            full = lax.dot_general(both, jac_ref[first + i], dims, preferred_element_type=jnp.float32)
            picked = jnp.where(rank == i, full, picked)
        return picked[:group] + picked[group:]

    def one(g, carry):
        first = pl.multiple_of(g * group, group)
        places = [slot_ref[first + i] for i in range(group)]
        states = jnp.concatenate([state_ref[pl.ds(p, 1), :] for p in places], axis=0)
        here = pl.ds(first, group)
        pred = product(states, first, (((1,), (1,)), ((), ())))
        weight = weight_ref[here, :] * valid_ref[here, :].astype(jnp.float32)
        terms = product(weight * (value_ref[here, :] - pred), first, (((1,), (0,)), ((), ())))
        for i, p in enumerate(places):
            out_ref[pl.ds(p, 1), :] = terms[i : i + 1]
        return carry

    lax.fori_loop(0, blocks // group, one, 0)


def block_terms(slot, states, jac, value, weight, valid):
    return pl.pallas_call(
        blocks_kernel,
        out_shape=jax.ShapeDtypeStruct(states.shape, jnp.float32),
        in_specs=[SMEM] + [VMEM] * 5,
        out_specs=VMEM,
        name="blocks",
    )(slot, states, jac, value, weight, valid)


def scatter_kernel(slots, ids_ref, terms_ref, out_ref):
    _, levels, nlon = out_ref.shape
    per_row = nlon // TW
    out_ref[...] = jnp.zeros_like(out_ref)
    lane = lax.broadcasted_iota(jnp.int32, (levels, LANES), 1)
    level = lax.broadcasted_iota(jnp.int32, (levels, LANES), 0)
    source = level * TW + lax.rem(lane, TW)
    owner = lane // TW

    def one(d, carry):
        for s in range(slots):
            row, start, offset = tile_place(ids_ref[d, s], per_row)
            spread = jnp.broadcast_to(terms_ref[d, s : s + 1, :], (levels, levels * TW))
            moved = jnp.take_along_axis(spread, source, axis=1)
            here = (row, slice(None), pl.ds(start, LANES))
            out_ref[here] = out_ref[here] + jnp.where(owner == offset // TW, moved, 0.0)
        return carry

    lax.fori_loop(0, terms_ref.shape[0], one, 0)


def scatter(ids, terms, shape, slots):
    return pl.pallas_call(
        functools.partial(scatter_kernel, slots),
        out_shape=jax.ShapeDtypeStruct(shape, jnp.float32),
        in_specs=[SMEM, VMEM],
        out_specs=VMEM,
        name="scatter",
    )(ids, terms)


def chain_kernel(
    sections, lats, coeff_ref, low_ref, high_ref, last_low_ref, last_high_ref, end_ref, forcing_ref, out_ref,
    main, low, high, edge_low, edge_high, ahead, weighted, partial, second,
    main_send, main_recv, down_send, up_send, low_recv, high_recv,
):
    section, band = lax.axis_index("tm"), lax.axis_index("lat")
    rows, levels, nlon = end_ref.shape
    chunks = levels // CHUNK
    is_last = section == sections - 1
    has_before, has_low, has_high = section > 0, band > 0, band < lats - 1

    sends_low, sends_high = has_low & jnp.logical_not(is_last), has_high & jnp.logical_not(is_last)

    barrier = pltpu.get_barrier_semaphore()
    sides = (
        (jnp.logical_not(is_last), section + 1, band),
        (has_before, section - 1, band),
        (has_low, section, band - 1),
        (has_high, section, band + 1),
    )
    for there, tm, lat in sides:
        @pl.when(there)
        def _(tm=tm, lat=lat):
            pl.semaphore_signal(barrier, inc=1, device_id=(tm, lat), device_id_type=MESH)
    pl.semaphore_wait(barrier, sum(there.astype(jnp.int32) for there, _, _ in sides))

    def remote(src, dst, send, recv, tm, lat):
        return pltpu.make_async_remote_copy(
            src_ref=src, dst_ref=dst, send_sem=send, recv_sem=recv, device_id=(tm, lat), device_id_type=MESH
        )

    def local_main(c):
        return pltpu.make_async_copy(
            end_ref.at[:, pl.ds(pl.multiple_of(c * CHUNK, CHUNK), CHUNK), :], main.at[c], main_recv.at[c]
        )

    def handed(c):
        return remote(ahead.at[c], main.at[c], main_send.at[c], main_recv.at[c], section - 1, band)

    def downward(c):
        return remote(edge_low.at[c], high.at[c], down_send.at[c], high_recv.at[c], section, band - 1)

    def upward(c):
        return remote(edge_high.at[c], low.at[c], up_send.at[c], low_recv.at[c], section, band + 1)

    @pl.when(jnp.logical_not(has_low))
    def _():
        low[...] = jnp.zeros_like(low)

    @pl.when(jnp.logical_not(has_high))
    def _():
        high[...] = jnp.zeros_like(high)

    @pl.when(is_last)
    def _():
        for c in range(chunks):
            local_main(c).start()
            low[c] = last_low_ref[:, c * CHUNK : (c + 1) * CHUNK, :]
            high[c] = last_high_ref[:, c * CHUNK : (c + 1) * CHUNK, :]

    def levels_of(c):
        return pl.ds(pl.multiple_of(c * CHUNK, CHUNK), CHUNK)

    def along(mid):
        return pltpu.roll(mid, 1, 1) + pltpu.roll(mid, nlon - 1, 1) - 4.0 * mid

    def begin(c):
        @pl.when(is_last)
        def _():
            local_main(c).wait()

        @pl.when(jnp.logical_not(is_last))
        def _():
            handed(c).wait_recv()

        span = levels_of(c)
        for r in range(rows):
            weighted[c, r] = coeff_ref[0, r, span, :] * main[c, r].astype(jnp.float32)
        for r in range(rows):
            mid = weighted[c, r]
            value = main[c, r].astype(jnp.float32) + along(mid)
            if r > 0:
                value = value + weighted[c, r - 1]
            if r < rows - 1:
                value = value + weighted[c, r + 1]
            partial[c, r] = value
            if r == 0:
                edge_low[c, 0] = mid.astype(jnp.bfloat16)
                edge_low[c, 1] = (coeff_ref[0, r, span, :] * value).astype(jnp.bfloat16)
            if r == rows - 1:
                edge_high[c, 0] = mid.astype(jnp.bfloat16)
                edge_high[c, 1] = (coeff_ref[0, r, span, :] * value).astype(jnp.bfloat16)

        @pl.when(sends_low)
        def _():
            downward(c).start()

        @pl.when(sends_high)
        def _():
            upward(c).start()

    def complete(c):
        span = levels_of(c)
        end = rows - 1
        partial[c, 0] = partial[c, 0] + low[c, 0].astype(jnp.float32)
        partial[c, end] = partial[c, end] + high[c, 0].astype(jnp.float32)
        second[0] = low[c, 1].astype(jnp.float32) + low_ref[0, span, :].astype(jnp.float32) * weighted[c, 0]
        second[rows + 1] = high[c, 1].astype(jnp.float32) + high_ref[0, span, :].astype(jnp.float32) * weighted[c, end]
        for r in range(rows):
            second[r + 1] = coeff_ref[0, r, span, :] * partial[c, r]
        for r in range(rows):
            value = partial[c, r] + second[r] + second[r + 2] + along(second[r + 1]) + forcing_ref[r, span, :]
            out_ref[0, r, span, :] = value
            ahead[c, r] = value.astype(jnp.bfloat16)

    begin(0)

    def step(c, carry):
        @pl.when(c + 1 < chunks)
        def _():
            begin(c + 1)

        @pl.when(sends_low)
        def _():
            upward(c).wait_recv()

        @pl.when(sends_high)
        def _():
            downward(c).wait_recv()

        complete(c)

        @pl.when(has_before)
        def _():
            handed(c).start()

        return carry

    lax.fori_loop(0, chunks, step, 0)

    def finish(c, carry):
        @pl.when(sends_low)
        def _():
            downward(c).wait_send()

        @pl.when(sends_high)
        def _():
            upward(c).wait_send()

        @pl.when(has_before)
        def _():
            handed(c).wait_send()

        return carry

    lax.fori_loop(0, chunks, finish, 0)


def chain(coeff, low, high, last_low, last_high, end, forcing):
    rows, levels, nlon = end.shape
    chunks = levels // CHUNK
    part = lambda n, kind: pltpu.VMEM((chunks, n, CHUNK, nlon), kind)
    return pl.pallas_call(
        functools.partial(chain_kernel, lax.axis_size("tm"), lax.axis_size("lat")),
        out_shape=jax.ShapeDtypeStruct(coeff.shape, jnp.float32),
        in_specs=[VMEM] * 7,
        out_specs=VMEM,
        scratch_shapes=[
            part(rows, jnp.bfloat16),
            part(SUB, jnp.bfloat16),
            part(SUB, jnp.bfloat16),
            part(SUB, jnp.bfloat16),
            part(SUB, jnp.bfloat16),
            part(rows, jnp.bfloat16),
            part(rows, jnp.float32),
            part(rows, jnp.float32),
            pltpu.VMEM((rows + 2, CHUNK, nlon), jnp.float32),
        ]
        + [pltpu.SemaphoreType.DMA((chunks,))] * 6,
        compiler_params=pltpu.CompilerParams(
            collective_id=9, has_side_effects=True, vmem_limit_bytes=48 * 1024 * 1024
        ),
        name="chain",
    )(coeff, low, high, last_low, last_high, end, forcing)


def per_device(
    trajectory,
    diffusivity,
    adjoint_end,
    obs_jac,
    obs_value,
    obs_weight,
    obs_valid,
    obs_owner,
    obs_tile,
):
    _, lat_dev, levels, nlon = trajectory.shape
    lats = lax.axis_size("lat")
    devices = lax.axis_size("tm") * lats
    blocks = obs_owner.shape[0]
    slots = max(2, 2 * blocks // devices)
    upward = [(i, i + 1) for i in range(lats - 1)]
    downward = [(i + 1, i) for i in range(lats - 1)]
    ids, slot = route(obs_owner[:, 0], obs_tile, devices, slots)
    wanted = exchange(ids[:, None, :], 1)[:, 0]
    edges = lax.optimization_barrier((diffusivity[0, :1], diffusivity[0, lat_dev - 1 :], wanted))
    wanted = edges[2]
    low = lax.ppermute(edges[1].astype(jnp.bfloat16), "lat", upward)
    high = lax.ppermute(edges[0].astype(jnp.bfloat16), "lat", downward)
    found = gather(wanted, trajectory, slots)
    edge_low, edge_high = last_edges(diffusivity, adjoint_end)
    returned, last_low = exchange(found, 2, edge_high, 1)
    terms = block_terms(
        slot, returned.reshape(devices * PAD, -1), obs_jac, obs_value, obs_weight, obs_valid
    )
    received, last_high = exchange(terms.reshape(found.shape), 3, edge_low, -1)
    forcing = scatter(wanted, received, (lat_dev, levels, nlon), slots)
    return chain(diffusivity, low, high, last_low, last_high, adjoint_end, forcing)


def solution(mesh):
    in_specs = (
        P("tm", "lat", None, None),
        P("tm", "lat", None, None),
        P("lat", None, None),
        P(("tm", "lat"), None, None),
        P(("tm", "lat"), None),
        P(("tm", "lat"), None),
        P(("tm", "lat"), None),
        P(("tm", "lat"), None),
        P(("tm", "lat")),
    )
    out_specs = P("tm", "lat", None, None)
    return jax.shard_map(
        per_device, mesh=mesh, in_specs=in_specs, out_specs=out_specs, check_vma=False
    )
```

```python
import functools

import jax
import jax.numpy as jnp
from jax import lax
from jax.experimental import pallas as pl
from jax.experimental.pallas import tpu as pltpu
from jax.sharding import PartitionSpec as P

TW = 2
SUB = 2
LANES = 128
PAD = 8
CHUNK = 8
MESH = pl.DeviceIdType.MESH
VMEM = pl.BlockSpec(memory_space=pltpu.VMEM)
SMEM = pl.BlockSpec(memory_space=pltpu.SMEM)


def route_kernel(slots, owner_ref, tile_ref, ids_ref, slot_ref, count_ref):
    devices = ids_ref.shape[0]

    def clear(d, carry):
        count_ref[d] = 0
        for s in range(slots):
            ids_ref[d, s] = 0
        return carry

    lax.fori_loop(0, devices, clear, 0)

    def place(k, carry):
        target = owner_ref[k]
        rank = count_ref[target]
        count_ref[target] = rank + 1
        ids_ref[target, rank] = tile_ref[k]
        slot_ref[k] = target * PAD + rank
        return carry

    lax.fori_loop(0, owner_ref.shape[0], place, 0)


def route(owner, tile, devices, slots):
    return pl.pallas_call(
        functools.partial(route_kernel, slots),
        out_shape=(
            jax.ShapeDtypeStruct((devices, LANES), jnp.int32),
            jax.ShapeDtypeStruct(owner.shape, jnp.int32),
        ),
        in_specs=[SMEM, SMEM],
        out_specs=(SMEM, SMEM),
        scratch_shapes=[pltpu.SMEM((devices,), jnp.int32)],
        name="route",
    )(owner, tile)


def exchange_kernel(count, lat, shift, *refs):
    if shift:
        x_ref, edge_ref, out_ref, beside_ref, send_sem, recv_sem, own_sem, edge_send, edge_recv = refs
    else:
        x_ref, out_ref, send_sem, recv_sem, own_sem = refs
    me = lax.axis_index("tm") * lat + lax.axis_index("lat")
    barrier = pltpu.get_barrier_semaphore()

    def greet(j, carry):
        to = lax.rem(me + j, count)
        pl.semaphore_signal(barrier, inc=1, device_id=(to // lat, lax.rem(to, lat)), device_id_type=MESH)
        return carry

    lax.fori_loop(1, count, greet, 0)
    own = pltpu.make_async_copy(x_ref.at[me], out_ref.at[me], own_sem)
    own.start()
    pl.semaphore_wait(barrier, count - 1)

    def outgoing(j):
        to = lax.rem(me + j, count)
        return pltpu.make_async_remote_copy(
            src_ref=x_ref.at[to],
            dst_ref=out_ref.at[me],
            send_sem=send_sem.at[j],
            recv_sem=recv_sem.at[j],
            device_id=(to // lat, lax.rem(to, lat)),
            device_id_type=MESH,
        )

    def incoming(j):
        source = lax.rem(me + count - j, count)
        return pltpu.make_async_remote_copy(
            src_ref=x_ref.at[source],
            dst_ref=out_ref.at[source],
            send_sem=send_sem.at[j],
            recv_sem=recv_sem.at[j],
            device_id=(source // lat, lax.rem(source, lat)),
            device_id_type=MESH,
        )

    def launch(j, carry):
        outgoing(j).start()
        return carry

    def land(j, carry):
        incoming(j).wait_recv()
        outgoing(j).wait_send()
        return carry

    lax.fori_loop(1, count, launch, 0)
    if shift:
        band, section = lax.axis_index("lat"), lax.axis_index("tm")
        is_last = section == count // lat - 1
        gives = is_last & (band < lat - 1 if shift > 0 else band > 0)
        takes = is_last & (band > 0 if shift > 0 else band < lat - 1)

        def edge():
            return pltpu.make_async_remote_copy(
                src_ref=edge_ref,
                dst_ref=beside_ref,
                send_sem=edge_send,
                recv_sem=edge_recv,
                device_id=(section, band + shift),
                device_id_type=MESH,
            )

        @pl.when(gives)
        def _():
            edge().start()

        @pl.when(jnp.logical_not(takes))
        def _():
            beside_ref[...] = jnp.zeros_like(beside_ref)

    own.wait()
    lax.fori_loop(1, count, land, 0)
    if shift:
        @pl.when(takes)
        def _():
            edge().wait_recv()

        @pl.when(gives)
        def _():
            edge().wait_send()


def last_edges_kernel(coeff_ref, end_ref, low_ref, high_ref, first_ref, final_ref):
    rows, levels, nlon = end_ref.shape

    def one(c, carry):
        span = pl.ds(pl.multiple_of(c * 16, 16), 16)

        def weigh(r):
            return coeff_ref[0, r, span, :] * end_ref[r, span, :].astype(jnp.float32)

        for r, inner, ref in ((0, 1, low_ref), (rows - 1, rows - 2, high_ref)):
            mid = weigh(r)
            value = end_ref[r, span, :].astype(jnp.float32) + weigh(inner)
            value = value + pltpu.roll(mid, 1, 1) + pltpu.roll(mid, nlon - 1, 1) - 4.0 * mid
            ref[0, span, :] = mid.astype(jnp.bfloat16)
            ref[1, span, :] = (coeff_ref[0, r, span, :] * value).astype(jnp.bfloat16)
        first_ref[0, span, :] = coeff_ref[0, 0, span, :].astype(jnp.bfloat16)
        final_ref[0, span, :] = coeff_ref[0, rows - 1, span, :].astype(jnp.bfloat16)
        return carry

    lax.fori_loop(0, levels // 16, one, 0)


def last_edges(coeff, end):
    edge = jax.ShapeDtypeStruct((2,) + end.shape[1:], jnp.bfloat16)
    single = jax.ShapeDtypeStruct((1,) + end.shape[1:], jnp.bfloat16)
    return pl.pallas_call(
        last_edges_kernel,
        out_shape=(edge, edge, single, single),
        in_specs=[VMEM, VMEM],
        out_specs=(VMEM,) * 4,
        name="last_edges",
    )(coeff, end)


def exchange(x, collective_id, edge=None, shift=0):
    lat = lax.axis_size("lat")
    count = lax.axis_size("tm") * lat
    if shift:
        return pl.pallas_call(
            functools.partial(exchange_kernel, count, lat, shift),
            out_shape=(jax.ShapeDtypeStruct(x.shape, x.dtype), jax.ShapeDtypeStruct(edge.shape, edge.dtype)),
            in_specs=[VMEM, VMEM],
            out_specs=(VMEM, VMEM),
            scratch_shapes=[pltpu.SemaphoreType.DMA((count,))] * 2 + [pltpu.SemaphoreType.DMA] * 3,
            compiler_params=pltpu.CompilerParams(collective_id=collective_id, has_side_effects=True),
            name="exchange%d" % collective_id,
        )(x, edge)
    return pl.pallas_call(
        functools.partial(exchange_kernel, count, lat, 0),
        out_shape=jax.ShapeDtypeStruct(x.shape, x.dtype),
        in_specs=[VMEM],
        out_specs=VMEM,
        scratch_shapes=[
            pltpu.SemaphoreType.DMA((count,)),
            pltpu.SemaphoreType.DMA((count,)),
            pltpu.SemaphoreType.DMA,
        ],
        compiler_params=pltpu.CompilerParams(collective_id=collective_id, has_side_effects=True),
        name="exchange%d" % collective_id,
    )(x)


def tile_place(tile, per_row):
    row = tile // per_row
    lon = (tile - row * per_row) * TW
    column = lon // LANES
    return row, pl.multiple_of(column * LANES, LANES), lon - column * LANES


def gather_kernel(slots, ids_ref, traj_ref, out_ref):
    _, _, levels, nlon = traj_ref.shape
    per_row = nlon // TW
    tile_len = levels * TW
    entry = lax.broadcasted_iota(jnp.int32, (levels, tile_len), 1)
    level = lax.broadcasted_iota(jnp.int32, (levels, tile_len), 0)
    part = lax.rem(entry, TW)
    keep = entry // TW == level
    zeros = jnp.zeros((PAD - slots, tile_len), jnp.float32)

    def one(d, carry):
        rows = []
        for s in range(slots):
            row, start, offset = tile_place(ids_ref[d, s], per_row)
            field = traj_ref[0, row, :, pl.ds(start, LANES)]
            picked = jnp.take_along_axis(field, part + offset, axis=1)
            rows.append(jnp.sum(jnp.where(keep, picked, 0.0), axis=0, keepdims=True))
        out_ref[d] = jnp.concatenate(rows + [zeros], axis=0)
        return carry

    lax.fori_loop(0, out_ref.shape[0], one, 0)


def gather(ids, traj, slots):
    devices = ids.shape[0]
    tile_len = traj.shape[2] * TW
    return pl.pallas_call(
        functools.partial(gather_kernel, slots),
        out_shape=jax.ShapeDtypeStruct((devices, PAD, tile_len), jnp.float32),
        in_specs=[SMEM, VMEM],
        out_specs=VMEM,
        name="gather",
    )(ids, traj)


def split(x):
    top = x.astype(jnp.bfloat16)
    rest = (x - top.astype(jnp.float32)).astype(jnp.bfloat16)
    return jnp.concatenate([top, rest], axis=0)


def blocks_kernel(slot_ref, state_ref, jac_ref, value_ref, weight_ref, valid_ref, out_ref):
    group = PAD
    blocks, _, tile_len = jac_ref.shape
    out_ref[...] = jnp.zeros_like(out_ref)
    rank = lax.rem(lax.broadcasted_iota(jnp.int32, (2 * group, tile_len), 0), group)

    def product(vectors, first, dims):
        both = split(vectors)
        picked = jnp.zeros((2 * group, tile_len), jnp.float32)
        for i in range(group):
            full = lax.dot_general(both, jac_ref[first + i], dims, preferred_element_type=jnp.float32)
            picked = jnp.where(rank == i, full, picked)
        return picked[:group] + picked[group:]

    def one(g, carry):
        first = pl.multiple_of(g * group, group)
        places = [slot_ref[first + i] for i in range(group)]
        states = jnp.concatenate([state_ref[pl.ds(p, 1), :] for p in places], axis=0)
        here = pl.ds(first, group)
        pred = product(states, first, (((1,), (1,)), ((), ())))
        weight = weight_ref[here, :] * valid_ref[here, :].astype(jnp.float32)
        terms = product(weight * (value_ref[here, :] - pred), first, (((1,), (0,)), ((), ())))
        for i, p in enumerate(places):
            out_ref[pl.ds(p, 1), :] = terms[i : i + 1]
        return carry

    lax.fori_loop(0, blocks // group, one, 0)


def block_terms(slot, states, jac, value, weight, valid):
    return pl.pallas_call(
        blocks_kernel,
        out_shape=jax.ShapeDtypeStruct(states.shape, jnp.float32),
        in_specs=[SMEM] + [VMEM] * 5,
        out_specs=VMEM,
        name="blocks",
    )(slot, states, jac, value, weight, valid)


def scatter_kernel(slots, ids_ref, terms_ref, out_ref):
    _, levels, nlon = out_ref.shape
    per_row = nlon // TW
    out_ref[...] = jnp.zeros_like(out_ref)
    lane = lax.broadcasted_iota(jnp.int32, (levels, LANES), 1)
    level = lax.broadcasted_iota(jnp.int32, (levels, LANES), 0)
    source = level * TW + lax.rem(lane, TW)
    owner = lane // TW

    def one(d, carry):
        for s in range(slots):
            row, start, offset = tile_place(ids_ref[d, s], per_row)
            spread = jnp.broadcast_to(terms_ref[d, s : s + 1, :], (levels, levels * TW))
            moved = jnp.take_along_axis(spread, source, axis=1)
            here = (row, slice(None), pl.ds(start, LANES))
            out_ref[here] = out_ref[here] + jnp.where(owner == offset // TW, moved, 0.0)
        return carry

    lax.fori_loop(0, terms_ref.shape[0], one, 0)


def scatter(ids, terms, shape, slots):
    return pl.pallas_call(
        functools.partial(scatter_kernel, slots),
        out_shape=jax.ShapeDtypeStruct(shape, jnp.float32),
        in_specs=[SMEM, VMEM],
        out_specs=VMEM,
        name="scatter",
    )(ids, terms)


def chain_kernel(
    sections, lats, coeff_ref, low_ref, high_ref, last_low_ref, last_high_ref, end_ref, forcing_ref, out_ref,
    main, low, high, edge_low, edge_high, ahead, weighted, partial, second,
    main_send, main_recv, down_send, up_send, low_recv, high_recv,
):
    section, band = lax.axis_index("tm"), lax.axis_index("lat")
    rows, levels, nlon = end_ref.shape
    chunks = levels // CHUNK
    is_last = section == sections - 1
    has_before, has_low, has_high = section > 0, band > 0, band < lats - 1

    sends_low, sends_high = has_low & jnp.logical_not(is_last), has_high & jnp.logical_not(is_last)

    barrier = pltpu.get_barrier_semaphore()
    sides = (
        (jnp.logical_not(is_last), section + 1, band),
        (has_before, section - 1, band),
        (has_low, section, band - 1),
        (has_high, section, band + 1),
    )
    for there, tm, lat in sides:
        @pl.when(there)
        def _(tm=tm, lat=lat):
            pl.semaphore_signal(barrier, inc=1, device_id=(tm, lat), device_id_type=MESH)
    pl.semaphore_wait(barrier, sum(there.astype(jnp.int32) for there, _, _ in sides))

    def remote(src, dst, send, recv, tm, lat):
        return pltpu.make_async_remote_copy(
            src_ref=src, dst_ref=dst, send_sem=send, recv_sem=recv, device_id=(tm, lat), device_id_type=MESH
        )

    def local_main(c):
        return pltpu.make_async_copy(
            end_ref.at[:, pl.ds(pl.multiple_of(c * CHUNK, CHUNK), CHUNK), :], main.at[c], main_recv.at[c]
        )

    def handed(c):
        return remote(ahead.at[c], main.at[c], main_send.at[c], main_recv.at[c], section - 1, band)

    def downward(c):
        return remote(edge_low.at[c], high.at[c], down_send.at[c], high_recv.at[c], section, band - 1)

    def upward(c):
        return remote(edge_high.at[c], low.at[c], up_send.at[c], low_recv.at[c], section, band + 1)

    @pl.when(jnp.logical_not(has_low))
    def _():
        low[...] = jnp.zeros_like(low)

    @pl.when(jnp.logical_not(has_high))
    def _():
        high[...] = jnp.zeros_like(high)

    @pl.when(is_last)
    def _():
        for c in range(chunks):
            local_main(c).start()
            low[c] = last_low_ref[:, c * CHUNK : (c + 1) * CHUNK, :]
            high[c] = last_high_ref[:, c * CHUNK : (c + 1) * CHUNK, :]

    def levels_of(c):
        return pl.ds(pl.multiple_of(c * CHUNK, CHUNK), CHUNK)

    def along(mid):
        return pltpu.roll(mid, 1, 1) + pltpu.roll(mid, nlon - 1, 1) - 4.0 * mid

    def begin(c):
        @pl.when(is_last)
        def _():
            local_main(c).wait()

        @pl.when(jnp.logical_not(is_last))
        def _():
            handed(c).wait_recv()

        span = levels_of(c)
        for r in range(rows):
            weighted[c, r] = coeff_ref[0, r, span, :] * main[c, r].astype(jnp.float32)
        for r in range(rows):
            mid = weighted[c, r]
            value = main[c, r].astype(jnp.float32) + along(mid)
            if r > 0:
                value = value + weighted[c, r - 1]
            if r < rows - 1:
                value = value + weighted[c, r + 1]
            partial[c, r] = value
            if r == 0:
                edge_low[c, 0] = mid.astype(jnp.bfloat16)
                edge_low[c, 1] = (coeff_ref[0, r, span, :] * value).astype(jnp.bfloat16)
            if r == rows - 1:
                edge_high[c, 0] = mid.astype(jnp.bfloat16)
                edge_high[c, 1] = (coeff_ref[0, r, span, :] * value).astype(jnp.bfloat16)

        @pl.when(sends_low)
        def _():
            downward(c).start()

        @pl.when(sends_high)
        def _():
            upward(c).start()

    def complete(c):
        span = levels_of(c)
        end = rows - 1
        partial[c, 0] = partial[c, 0] + low[c, 0].astype(jnp.float32)
        partial[c, end] = partial[c, end] + high[c, 0].astype(jnp.float32)
        second[0] = low[c, 1].astype(jnp.float32) + low_ref[0, span, :].astype(jnp.float32) * weighted[c, 0]
        second[rows + 1] = high[c, 1].astype(jnp.float32) + high_ref[0, span, :].astype(jnp.float32) * weighted[c, end]
        for r in range(rows):
            second[r + 1] = coeff_ref[0, r, span, :] * partial[c, r]
        for r in range(rows):
            value = partial[c, r] + second[r] + second[r + 2] + along(second[r + 1]) + forcing_ref[r, span, :]
            out_ref[0, r, span, :] = value
            ahead[c, r] = value.astype(jnp.bfloat16)

    look = jnp.where(section == sections - 2, min(4, chunks), min(2, chunks))

    def open_one(c, carry):
        begin(c)
        return carry

    lax.fori_loop(0, look, open_one, 0)

    def step(c, carry):
        @pl.when(c + look < chunks)
        def _():
            begin(c + look)

        @pl.when(sends_low)
        def _():
            upward(c).wait_recv()

        @pl.when(sends_high)
        def _():
            downward(c).wait_recv()

        complete(c)

        @pl.when(has_before)
        def _():
            handed(c).start()

        return carry

    lax.fori_loop(0, chunks, step, 0)

    def finish(c, carry):
        @pl.when(sends_low)
        def _():
            downward(c).wait_send()

        @pl.when(sends_high)
        def _():
            upward(c).wait_send()

        @pl.when(has_before)
        def _():
            handed(c).wait_send()

        return carry

    lax.fori_loop(0, chunks, finish, 0)


def chain(coeff, low, high, last_low, last_high, end, forcing):
    rows, levels, nlon = end.shape
    chunks = levels // CHUNK
    part = lambda n, kind: pltpu.VMEM((chunks, n, CHUNK, nlon), kind)
    return pl.pallas_call(
        functools.partial(chain_kernel, lax.axis_size("tm"), lax.axis_size("lat")),
        out_shape=jax.ShapeDtypeStruct(coeff.shape, jnp.float32),
        in_specs=[VMEM] * 7,
        out_specs=VMEM,
        scratch_shapes=[
            part(rows, jnp.bfloat16),
            part(SUB, jnp.bfloat16),
            part(SUB, jnp.bfloat16),
            part(SUB, jnp.bfloat16),
            part(SUB, jnp.bfloat16),
            part(rows, jnp.bfloat16),
            part(rows, jnp.float32),
            part(rows, jnp.float32),
            pltpu.VMEM((rows + 2, CHUNK, nlon), jnp.float32),
        ]
        + [pltpu.SemaphoreType.DMA((chunks,))] * 6,
        compiler_params=pltpu.CompilerParams(
            collective_id=9, has_side_effects=True, vmem_limit_bytes=48 * 1024 * 1024
        ),
        name="chain",
    )(coeff, low, high, last_low, last_high, end, forcing)


def per_device(
    trajectory,
    diffusivity,
    adjoint_end,
    obs_jac,
    obs_value,
    obs_weight,
    obs_valid,
    obs_owner,
    obs_tile,
):
    _, lat_dev, levels, nlon = trajectory.shape
    lats = lax.axis_size("lat")
    devices = lax.axis_size("tm") * lats
    blocks = obs_owner.shape[0]
    slots = max(2, 2 * blocks // devices)
    upward = [(i, i + 1) for i in range(lats - 1)]
    downward = [(i + 1, i) for i in range(lats - 1)]
    ids, slot = route(obs_owner[:, 0], obs_tile, devices, slots)
    wanted = exchange(ids[:, None, :], 1)[:, 0]
    edge_low, edge_high, first_row, final_row = last_edges(diffusivity, adjoint_end)
    edges = lax.optimization_barrier((first_row, final_row, wanted))
    wanted = edges[2]
    low = lax.ppermute(edges[1], "lat", upward)
    high = lax.ppermute(edges[0], "lat", downward)
    found = gather(wanted, trajectory, slots)
    returned, last_low = exchange(found, 2, edge_high, 1)
    terms = block_terms(
        slot, returned.reshape(devices * PAD, -1), obs_jac, obs_value, obs_weight, obs_valid
    )
    received, last_high = exchange(terms.reshape(found.shape), 3, edge_low, -1)
    forcing = scatter(wanted, received, (lat_dev, levels, nlon), slots)
    return chain(diffusivity, low, high, last_low, last_high, adjoint_end, forcing)


def solution(mesh):
    in_specs = (
        P("tm", "lat", None, None),
        P("tm", "lat", None, None),
        P("lat", None, None),
        P(("tm", "lat"), None, None),
        P(("tm", "lat"), None),
        P(("tm", "lat"), None),
        P(("tm", "lat"), None),
        P(("tm", "lat"), None),
        P(("tm", "lat")),
    )
    out_specs = P("tm", "lat", None, None)
    return jax.shard_map(
        per_device, mesh=mesh, in_specs=in_specs, out_specs=out_specs, check_vma=False
    )
```

```python
import functools

import jax
import jax.numpy as jnp
from jax import lax
from jax.experimental import pallas as pl
from jax.experimental.pallas import tpu as pltpu
from jax.sharding import PartitionSpec as P

TW = 2
SUB = 2
LANES = 128
PAD = 8
CHUNK = 16
MESH = pl.DeviceIdType.MESH
VMEM = pl.BlockSpec(memory_space=pltpu.VMEM)
SMEM = pl.BlockSpec(memory_space=pltpu.SMEM)


def route_kernel(slots, owner_ref, tile_ref, ids_ref, slot_ref, count_ref):
    devices = ids_ref.shape[0]

    def clear(d, carry):
        count_ref[d] = 0
        for s in range(slots):
            ids_ref[d, s] = 0
        return carry

    lax.fori_loop(0, devices, clear, 0)

    def place(k, carry):
        target = owner_ref[k]
        rank = count_ref[target]
        count_ref[target] = rank + 1
        ids_ref[target, rank] = tile_ref[k]
        slot_ref[k] = target * PAD + rank
        return carry

    lax.fori_loop(0, owner_ref.shape[0], place, 0)


def route(owner, tile, devices, slots):
    return pl.pallas_call(
        functools.partial(route_kernel, slots),
        out_shape=(
            jax.ShapeDtypeStruct((devices, LANES), jnp.int32),
            jax.ShapeDtypeStruct(owner.shape, jnp.int32),
        ),
        in_specs=[SMEM, SMEM],
        out_specs=(SMEM, SMEM),
        scratch_shapes=[pltpu.SMEM((devices,), jnp.int32)],
        name="route",
    )(owner, tile)


def exchange_kernel(count, lat, shift, *refs):
    if shift:
        x_ref, edge_ref, out_ref, beside_ref, send_sem, recv_sem, own_sem, edge_send, edge_recv = refs
    else:
        x_ref, out_ref, send_sem, recv_sem, own_sem = refs
    me = lax.axis_index("tm") * lat + lax.axis_index("lat")
    barrier = pltpu.get_barrier_semaphore()

    def greet(j, carry):
        to = lax.rem(me + j, count)
        pl.semaphore_signal(barrier, inc=1, device_id=(to // lat, lax.rem(to, lat)), device_id_type=MESH)
        return carry

    lax.fori_loop(1, count, greet, 0)
    own = pltpu.make_async_copy(x_ref.at[me], out_ref.at[me], own_sem)
    own.start()
    pl.semaphore_wait(barrier, count - 1)

    def outgoing(j):
        to = lax.rem(me + j, count)
        return pltpu.make_async_remote_copy(
            src_ref=x_ref.at[to],
            dst_ref=out_ref.at[me],
            send_sem=send_sem.at[j],
            recv_sem=recv_sem.at[j],
            device_id=(to // lat, lax.rem(to, lat)),
            device_id_type=MESH,
        )

    def incoming(j):
        source = lax.rem(me + count - j, count)
        return pltpu.make_async_remote_copy(
            src_ref=x_ref.at[source],
            dst_ref=out_ref.at[source],
            send_sem=send_sem.at[j],
            recv_sem=recv_sem.at[j],
            device_id=(source // lat, lax.rem(source, lat)),
            device_id_type=MESH,
        )

    def launch(j, carry):
        outgoing(j).start()
        return carry

    def land(j, carry):
        incoming(j).wait_recv()
        outgoing(j).wait_send()
        return carry

    lax.fori_loop(1, count, launch, 0)
    if shift:
        band, section = lax.axis_index("lat"), lax.axis_index("tm")
        is_last = section == count // lat - 1
        gives = is_last & (band < lat - 1 if shift > 0 else band > 0)
        takes = is_last & (band > 0 if shift > 0 else band < lat - 1)

        def edge():
            return pltpu.make_async_remote_copy(
                src_ref=edge_ref,
                dst_ref=beside_ref,
                send_sem=edge_send,
                recv_sem=edge_recv,
                device_id=(section, band + shift),
                device_id_type=MESH,
            )

        @pl.when(gives)
        def _():
            edge().start()

        @pl.when(jnp.logical_not(takes))
        def _():
            beside_ref[...] = jnp.zeros_like(beside_ref)

    own.wait()
    lax.fori_loop(1, count, land, 0)
    if shift:
        @pl.when(takes)
        def _():
            edge().wait_recv()

        @pl.when(gives)
        def _():
            edge().wait_send()


def last_edges_kernel(coeff_ref, end_ref, low_ref, high_ref, first_ref, final_ref):
    rows, levels, nlon = end_ref.shape

    def one(c, carry):
        span = pl.ds(pl.multiple_of(c * 16, 16), 16)

        def weigh(r):
            return coeff_ref[0, r, span, :] * end_ref[r, span, :].astype(jnp.float32)

        for r, inner, ref in ((0, 1, low_ref), (rows - 1, rows - 2, high_ref)):
            mid = weigh(r)
            value = end_ref[r, span, :].astype(jnp.float32) + weigh(inner)
            value = value + pltpu.roll(mid, 1, 1) + pltpu.roll(mid, nlon - 1, 1) - 4.0 * mid
            ref[0, span, :] = mid.astype(jnp.bfloat16)
            ref[1, span, :] = (coeff_ref[0, r, span, :] * value).astype(jnp.bfloat16)
        first_ref[0, span, :] = coeff_ref[0, 0, span, :].astype(jnp.bfloat16)
        final_ref[0, span, :] = coeff_ref[0, rows - 1, span, :].astype(jnp.bfloat16)
        return carry

    lax.fori_loop(0, levels // 16, one, 0)


def last_edges(coeff, end):
    edge = jax.ShapeDtypeStruct((2,) + end.shape[1:], jnp.bfloat16)
    single = jax.ShapeDtypeStruct((1,) + end.shape[1:], jnp.bfloat16)
    return pl.pallas_call(
        last_edges_kernel,
        out_shape=(edge, edge, single, single),
        in_specs=[VMEM, VMEM],
        out_specs=(VMEM,) * 4,
        name="last_edges",
    )(coeff, end)


def exchange(x, collective_id, edge=None, shift=0):
    lat = lax.axis_size("lat")
    count = lax.axis_size("tm") * lat
    if shift:
        return pl.pallas_call(
            functools.partial(exchange_kernel, count, lat, shift),
            out_shape=(jax.ShapeDtypeStruct(x.shape, x.dtype), jax.ShapeDtypeStruct(edge.shape, edge.dtype)),
            in_specs=[VMEM, VMEM],
            out_specs=(VMEM, VMEM),
            scratch_shapes=[pltpu.SemaphoreType.DMA((count,))] * 2 + [pltpu.SemaphoreType.DMA] * 3,
            compiler_params=pltpu.CompilerParams(collective_id=collective_id, has_side_effects=True),
            name="exchange%d" % collective_id,
        )(x, edge)
    return pl.pallas_call(
        functools.partial(exchange_kernel, count, lat, 0),
        out_shape=jax.ShapeDtypeStruct(x.shape, x.dtype),
        in_specs=[VMEM],
        out_specs=VMEM,
        scratch_shapes=[
            pltpu.SemaphoreType.DMA((count,)),
            pltpu.SemaphoreType.DMA((count,)),
            pltpu.SemaphoreType.DMA,
        ],
        compiler_params=pltpu.CompilerParams(collective_id=collective_id, has_side_effects=True),
        name="exchange%d" % collective_id,
    )(x)


def tile_place(tile, per_row):
    row = tile // per_row
    lon = (tile - row * per_row) * TW
    column = lon // LANES
    return row, pl.multiple_of(column * LANES, LANES), lon - column * LANES


def gather_kernel(slots, ids_ref, traj_ref, out_ref):
    _, _, levels, nlon = traj_ref.shape
    per_row = nlon // TW
    tile_len = levels * TW
    entry = lax.broadcasted_iota(jnp.int32, (levels, tile_len), 1)
    level = lax.broadcasted_iota(jnp.int32, (levels, tile_len), 0)
    part = lax.rem(entry, TW)
    keep = entry // TW == level
    zeros = jnp.zeros((PAD - slots, tile_len), jnp.float32)

    def one(d, carry):
        rows = []
        for s in range(slots):
            row, start, offset = tile_place(ids_ref[d, s], per_row)
            field = traj_ref[0, row, :, pl.ds(start, LANES)]
            picked = jnp.take_along_axis(field, part + offset, axis=1)
            rows.append(jnp.sum(jnp.where(keep, picked, 0.0), axis=0, keepdims=True))
        out_ref[d] = jnp.concatenate(rows + [zeros], axis=0)
        return carry

    lax.fori_loop(0, out_ref.shape[0], one, 0)


def gather(ids, traj, slots):
    devices = ids.shape[0]
    tile_len = traj.shape[2] * TW
    return pl.pallas_call(
        functools.partial(gather_kernel, slots),
        out_shape=jax.ShapeDtypeStruct((devices, PAD, tile_len), jnp.float32),
        in_specs=[SMEM, VMEM],
        out_specs=VMEM,
        name="gather",
    )(ids, traj)


def split(x):
    top = x.astype(jnp.bfloat16)
    rest = (x - top.astype(jnp.float32)).astype(jnp.bfloat16)
    return jnp.concatenate([top, rest], axis=0)


def blocks_kernel(slot_ref, state_ref, jac_ref, value_ref, weight_ref, valid_ref, out_ref):
    group = PAD
    blocks, _, tile_len = jac_ref.shape
    out_ref[...] = jnp.zeros_like(out_ref)
    rank = lax.rem(lax.broadcasted_iota(jnp.int32, (2 * group, tile_len), 0), group)

    def product(vectors, first, dims):
        both = split(vectors)
        picked = jnp.zeros((2 * group, tile_len), jnp.float32)
        for i in range(group):
            full = lax.dot_general(both, jac_ref[first + i], dims, preferred_element_type=jnp.float32)
            picked = jnp.where(rank == i, full, picked)
        return picked[:group] + picked[group:]

    def one(g, carry):
        first = pl.multiple_of(g * group, group)
        places = [slot_ref[first + i] for i in range(group)]
        states = jnp.concatenate([state_ref[pl.ds(p, 1), :] for p in places], axis=0)
        here = pl.ds(first, group)
        pred = product(states, first, (((1,), (1,)), ((), ())))
        weight = weight_ref[here, :] * valid_ref[here, :].astype(jnp.float32)
        terms = product(weight * (value_ref[here, :] - pred), first, (((1,), (0,)), ((), ())))
        for i, p in enumerate(places):
            out_ref[pl.ds(p, 1), :] = terms[i : i + 1]
        return carry

    lax.fori_loop(0, blocks // group, one, 0)


def block_terms(slot, states, jac, value, weight, valid):
    return pl.pallas_call(
        blocks_kernel,
        out_shape=jax.ShapeDtypeStruct(states.shape, jnp.float32),
        in_specs=[SMEM] + [VMEM] * 5,
        out_specs=VMEM,
        name="blocks",
    )(slot, states, jac, value, weight, valid)


def scatter_kernel(slots, ids_ref, terms_ref, out_ref):
    _, levels, nlon = out_ref.shape
    per_row = nlon // TW
    out_ref[...] = jnp.zeros_like(out_ref)
    lane = lax.broadcasted_iota(jnp.int32, (levels, LANES), 1)
    level = lax.broadcasted_iota(jnp.int32, (levels, LANES), 0)
    source = level * TW + lax.rem(lane, TW)
    owner = lane // TW

    def one(d, carry):
        for s in range(slots):
            row, start, offset = tile_place(ids_ref[d, s], per_row)
            spread = jnp.broadcast_to(terms_ref[d, s : s + 1, :], (levels, levels * TW))
            moved = jnp.take_along_axis(spread, source, axis=1)
            here = (row, slice(None), pl.ds(start, LANES))
            out_ref[here] = out_ref[here] + jnp.where(owner == offset // TW, moved, 0.0)
        return carry

    lax.fori_loop(0, terms_ref.shape[0], one, 0)


def scatter(ids, terms, shape, slots):
    return pl.pallas_call(
        functools.partial(scatter_kernel, slots),
        out_shape=jax.ShapeDtypeStruct(shape, jnp.float32),
        in_specs=[SMEM, VMEM],
        out_specs=VMEM,
        name="scatter",
    )(ids, terms)


def chain_kernel(
    sections, lats, coeff_ref, low_ref, high_ref, last_low_ref, last_high_ref, end_ref, forcing_ref, out_ref,
    main, low, high, edge_low, edge_high, ahead, weighted, partial, second,
    main_send, main_recv, down_send, up_send, low_recv, high_recv,
):
    section, band = lax.axis_index("tm"), lax.axis_index("lat")
    rows, levels, nlon = end_ref.shape
    chunks = levels // CHUNK
    is_last = section == sections - 1
    has_before, has_low, has_high = section > 0, band > 0, band < lats - 1

    sends_low, sends_high = has_low & jnp.logical_not(is_last), has_high & jnp.logical_not(is_last)

    barrier = pltpu.get_barrier_semaphore()
    sides = (
        (jnp.logical_not(is_last), section + 1, band),
        (has_before, section - 1, band),
        (has_low, section, band - 1),
        (has_high, section, band + 1),
    )
    for there, tm, lat in sides:
        @pl.when(there)
        def _(tm=tm, lat=lat):
            pl.semaphore_signal(barrier, inc=1, device_id=(tm, lat), device_id_type=MESH)
    pl.semaphore_wait(barrier, sum(there.astype(jnp.int32) for there, _, _ in sides))

    def remote(src, dst, send, recv, tm, lat):
        return pltpu.make_async_remote_copy(
            src_ref=src, dst_ref=dst, send_sem=send, recv_sem=recv, device_id=(tm, lat), device_id_type=MESH
        )

    def local_main(c):
        return pltpu.make_async_copy(
            end_ref.at[:, pl.ds(pl.multiple_of(c * CHUNK, CHUNK), CHUNK), :], main.at[c], main_recv.at[c]
        )

    def handed(c):
        return remote(ahead.at[c], main.at[c], main_send.at[c], main_recv.at[c], section - 1, band)

    def downward(c):
        return remote(edge_low.at[c], high.at[c], down_send.at[c], high_recv.at[c], section, band - 1)

    def upward(c):
        return remote(edge_high.at[c], low.at[c], up_send.at[c], low_recv.at[c], section, band + 1)

    @pl.when(jnp.logical_not(has_low))
    def _():
        low[...] = jnp.zeros_like(low)

    @pl.when(jnp.logical_not(has_high))
    def _():
        high[...] = jnp.zeros_like(high)

    @pl.when(is_last)
    def _():
        for c in range(chunks):
            local_main(c).start()
            low[c] = last_low_ref[:, c * CHUNK : (c + 1) * CHUNK, :]
            high[c] = last_high_ref[:, c * CHUNK : (c + 1) * CHUNK, :]

    def levels_of(c):
        return pl.ds(pl.multiple_of(c * CHUNK, CHUNK), CHUNK)

    def along(mid):
        return pltpu.roll(mid, 1, 1) + pltpu.roll(mid, nlon - 1, 1) - 4.0 * mid

    def begin(c):
        @pl.when(is_last)
        def _():
            local_main(c).wait()

        @pl.when(jnp.logical_not(is_last))
        def _():
            handed(c).wait_recv()

        span = levels_of(c)
        for r in range(rows):
            weighted[c, r] = coeff_ref[0, r, span, :] * main[c, r].astype(jnp.float32)
        for r in range(rows):
            mid = weighted[c, r]
            value = main[c, r].astype(jnp.float32) + along(mid)
            if r > 0:
                value = value + weighted[c, r - 1]
            if r < rows - 1:
                value = value + weighted[c, r + 1]
            partial[c, r] = value
            if r == 0:
                edge_low[c, 0] = mid.astype(jnp.bfloat16)
                edge_low[c, 1] = (coeff_ref[0, r, span, :] * value).astype(jnp.bfloat16)
            if r == rows - 1:
                edge_high[c, 0] = mid.astype(jnp.bfloat16)
                edge_high[c, 1] = (coeff_ref[0, r, span, :] * value).astype(jnp.bfloat16)

        @pl.when(sends_low)
        def _():
            downward(c).start()

        @pl.when(sends_high)
        def _():
            upward(c).start()

    def complete(c):
        span = levels_of(c)
        end = rows - 1
        partial[c, 0] = partial[c, 0] + low[c, 0].astype(jnp.float32)
        partial[c, end] = partial[c, end] + high[c, 0].astype(jnp.float32)
        second[0] = low[c, 1].astype(jnp.float32) + low_ref[0, span, :].astype(jnp.float32) * weighted[c, 0]
        second[rows + 1] = high[c, 1].astype(jnp.float32) + high_ref[0, span, :].astype(jnp.float32) * weighted[c, end]
        for r in range(rows):
            second[r + 1] = coeff_ref[0, r, span, :] * partial[c, r]
        for r in range(rows):
            value = partial[c, r] + second[r] + second[r + 2] + along(second[r + 1]) + forcing_ref[r, span, :]
            out_ref[0, r, span, :] = value
            ahead[c, r] = value.astype(jnp.bfloat16)

    look = jnp.where(section == sections - 2, min(4, chunks), min(2, chunks))

    def open_one(c, carry):
        begin(c)
        return carry

    lax.fori_loop(0, look, open_one, 0)

    def step(c, carry):
        @pl.when(c + look < chunks)
        def _():
            begin(c + look)

        @pl.when(sends_low)
        def _():
            upward(c).wait_recv()

        @pl.when(sends_high)
        def _():
            downward(c).wait_recv()

        complete(c)

        @pl.when(has_before)
        def _():
            handed(c).start()

        return carry

    lax.fori_loop(0, chunks, step, 0)

    def finish(c, carry):
        @pl.when(sends_low)
        def _():
            downward(c).wait_send()

        @pl.when(sends_high)
        def _():
            upward(c).wait_send()

        @pl.when(has_before)
        def _():
            handed(c).wait_send()

        return carry

    lax.fori_loop(0, chunks, finish, 0)


def chain(coeff, low, high, last_low, last_high, end, forcing):
    rows, levels, nlon = end.shape
    chunks = levels // CHUNK
    part = lambda n, kind: pltpu.VMEM((chunks, n, CHUNK, nlon), kind)
    return pl.pallas_call(
        functools.partial(chain_kernel, lax.axis_size("tm"), lax.axis_size("lat")),
        out_shape=jax.ShapeDtypeStruct(coeff.shape, jnp.float32),
        in_specs=[VMEM] * 7,
        out_specs=VMEM,
        scratch_shapes=[
            part(rows, jnp.bfloat16),
            part(SUB, jnp.bfloat16),
            part(SUB, jnp.bfloat16),
            part(SUB, jnp.bfloat16),
            part(SUB, jnp.bfloat16),
            part(rows, jnp.bfloat16),
            part(rows, jnp.float32),
            part(rows, jnp.float32),
            pltpu.VMEM((rows + 2, CHUNK, nlon), jnp.float32),
        ]
        + [pltpu.SemaphoreType.DMA((chunks,))] * 6,
        compiler_params=pltpu.CompilerParams(
            collective_id=9, has_side_effects=True, vmem_limit_bytes=48 * 1024 * 1024
        ),
        name="chain",
    )(coeff, low, high, last_low, last_high, end, forcing)


def per_device(
    trajectory,
    diffusivity,
    adjoint_end,
    obs_jac,
    obs_value,
    obs_weight,
    obs_valid,
    obs_owner,
    obs_tile,
):
    _, lat_dev, levels, nlon = trajectory.shape
    lats = lax.axis_size("lat")
    devices = lax.axis_size("tm") * lats
    blocks = obs_owner.shape[0]
    slots = max(2, 2 * blocks // devices)
    upward = [(i, i + 1) for i in range(lats - 1)]
    downward = [(i + 1, i) for i in range(lats - 1)]
    ids, slot = route(obs_owner[:, 0], obs_tile, devices, slots)
    wanted = exchange(ids[:, None, :], 1)[:, 0]
    edge_low, edge_high, first_row, final_row = last_edges(diffusivity, adjoint_end)
    edges = lax.optimization_barrier((first_row, final_row, wanted))
    wanted = edges[2]
    low = lax.ppermute(edges[1], "lat", upward)
    high = lax.ppermute(edges[0], "lat", downward)
    found = gather(wanted, trajectory, slots)
    returned, last_low = exchange(found, 2, edge_high, 1)
    terms = block_terms(
        slot, returned.reshape(devices * PAD, -1), obs_jac, obs_value, obs_weight, obs_valid
    )
    received, last_high = exchange(terms.reshape(found.shape), 3, edge_low, -1)
    forcing = scatter(wanted, received, (lat_dev, levels, nlon), slots)
    return chain(diffusivity, low, high, last_low, last_high, adjoint_end, forcing)


def solution(mesh):
    in_specs = (
        P("tm", "lat", None, None),
        P("tm", "lat", None, None),
        P("lat", None, None),
        P(("tm", "lat"), None, None),
        P(("tm", "lat"), None),
        P(("tm", "lat"), None),
        P(("tm", "lat"), None),
        P(("tm", "lat"), None),
        P(("tm", "lat")),
    )
    out_specs = P("tm", "lat", None, None)
    return jax.shard_map(
        per_device, mesh=mesh, in_specs=in_specs, out_specs=out_specs, check_vma=False
    )
```
